32 devices in a mesh: gx: 2 (over x), gy: 4 (over y, core), gz: 4 (over z).
Axes of the slice: x: 2, y: 2, z: 4, core: 2. Of those that a mesh axis runs over, the one named last changes fastest.
Arguments:
- right_side: float32 [24, 64, 512], P('gx', 'gy', 'gz'), may hold values from -8 to 8
- coefficient: float32 [24, 64, 512], P('gx', 'gy', 'gz'), may hold values from 0.02 to 1
Outputs:
- solution: float32 [24, 64, 512], P('gx', 'gy', 'gz')
- residual: float32 [24, 64, 512], P('gx', 'gy', 'gz')
- precond: float32 [24, 64, 512], P('gx', 'gy', 'gz')
- image: float32 [24, 64, 512], P('gx', 'gy', 'gz')
The draws below stay inside these ranges and needn't reach their ends.
All inputs are finite; a program needn't handle non-finite values.
Results may differ from the reference program's by a relative error of at most 0.00021.
Values sent between devices are 32-bit elements; how exact they have to be, the bound alone decides.
No kernel may reach another device: no remote copies, remote signals or barrier semaphores. Data moves between devices by JAX's collectives and lax.ppermute only.
A program may use at most 64 MiB of HBM per device.

```python
import math
import jax
import jax.numpy as jnp

SWEEPS = 4
ITERS = 1
NX = 24
NY = 64
NZ = 512


def block_levels(own_key, shape, shards, smallest, largest):
    loudness, own = 1.0, jax.random.fold_in(own_key, 6)
    for position, parts in shards:
        steps = jnp.exp(jax.random.uniform(jax.random.fold_in(own, position), (parts,), jnp.float32, smallest / len(shards), largest / len(shards)))
        loudness = loudness * jnp.repeat(steps, shape[position] // parts).reshape([-1 if axis == position else 1 for axis in range(len(shape))])
    return loudness


def noise(own_key, shape, scale, reach, pieces=(), kind=jnp.bfloat16):
    values = jax.random.normal(own_key, shape, jnp.float32) * scale
    if len(pieces) > 0:
        values = block_levels(own_key, shape, pieces, -0.22, 0.18) * values
    return jnp.clip(values, min=-reach, max=reach).astype(kind)


def setup_inputs(seed: int = 0) -> dict:
    arg_keys = jax.random.split(jax.random.key(seed), 3)
    return {
        "right_side": noise(arg_keys[0], (NX, NY, NZ), 1.0, 8.0, ((0, 2), (1, 4), (2, 4)), jnp.float32),
        "coefficient": jnp.clip(jnp.exp(math.log(1.0) - 3.912023 * jax.random.uniform(arg_keys[1], (NX, NY, NZ), jnp.float32) ** block_levels(arg_keys[1], (NX, NY, NZ), ((0, 2), (1, 4), (2, 4)), -0.2, 0.2)), 0.02, 1.0),
    }


relaxation = 0.6


def block_sum(padded):
    summed = padded[:-2] + padded[1:-1] + padded[2:]
    summed = summed[:, :-2] + summed[:, 1:-1] + summed[:, 2:]
    return summed[:, :, :-2] + summed[:, :, 1:-1] + summed[:, :, 2:]


def operate(values, reaction):
    return (27.0 + reaction) * values - block_sum(jnp.pad(values, 1))


def restrict(values):
    extent = values.shape
    grouped = values.reshape(extent[0] // 2, 2, extent[1] // 2, 2, extent[2] // 2, 2)
    return 0.5 * grouped.sum(axis=(1, 3, 5))


def prolong(values):
    return jnp.repeat(jnp.repeat(jnp.repeat(values, 2, axis=0), 2, axis=1), 2, axis=2)


def coarsest(source, reaction):
    correction = relaxation * source / (26.0 + reaction)
    for sweep in range(SWEEPS - 1):
        correction = correction + relaxation * (source - operate(correction, reaction)) / (26.0 + reaction)
    return correction


def multigrid(source, reactions, level_index):
    if level_index == 2:
        return coarsest(source, reactions[2])
    reaction = reactions[level_index]
    correction = relaxation * source / (26.0 + reaction)
    remainder = source - operate(correction, reaction)
    correction = correction + prolong(multigrid(restrict(remainder), reactions, level_index + 1))
    return correction + relaxation * (source - operate(correction, reaction)) / (26.0 + reaction)


def reference(right_side, coefficient):
    middle = restrict(coefficient)
    reactions = (coefficient, middle, restrict(middle))
    solution = jnp.zeros_like(right_side)
    residual = right_side
    precond = multigrid(residual, reactions, 0)
    image = operate(precond, coefficient)
    direction = precond
    dir_image = image
    dir_precond = precond
    dir_twice = image
    gamma_prev = jnp.float32(1.0)
    alpha_prev = jnp.float32(1.0)
    for step in range(ITERS):
        gamma_now = jnp.sum(residual * precond)
        delta_now = jnp.sum(image * precond)
        precond_image = multigrid(image, reactions, 0)
        image_twice = operate(precond_image, coefficient)
        if step == 0:
            alpha_now = gamma_now / delta_now
            direction = precond
            dir_image = image
            dir_precond = precond_image
            dir_twice = image_twice
        else:
            beta_now = gamma_now / gamma_prev
            alpha_now = gamma_now / (delta_now - beta_now * gamma_now / alpha_prev)
            dir_twice = image_twice + beta_now * dir_twice
            dir_precond = precond_image + beta_now * dir_precond
            dir_image = image + beta_now * dir_image
            direction = precond + beta_now * direction
        solution = solution + alpha_now * direction
        residual = residual - alpha_now * dir_image
        precond = precond - alpha_now * dir_precond
        image = image - alpha_now * dir_twice
        gamma_prev = gamma_now
        alpha_prev = alpha_now
    return (solution, residual, precond, image)
```

```python
import jax
import jax.numpy as jnp
from jax import lax
from jax.experimental import pallas as pl
from jax.experimental.pallas import tpu as pltpu
from jax.sharding import PartitionSpec as P

SWEEPS = 4
relaxation = 0.6
f32 = jnp.float32

HALO = 4


def roll(value, shift, axis):
    return pltpu.roll(value, shift % value.shape[axis], axis)


def iota(shape, axis):
    return lax.broadcasted_iota(jnp.int32, shape, axis)


class Shape:
    def __init__(self, nx, ny, nz, block):
        self.nx, self.ny, self.nz = nx, ny, nz
        self.bx, self.by, self.bz = block
        self.half = self.by // 2
        self.slots = nx * 4
        self.rows = self.bx * self.half
        self.x1 = nx * self.bx // 2
        self.y1 = self.half // 2
        self.slots1 = 2 * ny
        self.rows1 = self.x1 * self.y1
        self.share = 2 * self.rows1


def fine_tools(s):
    shape = (s.slots, s.bz)
    sub = iota(shape, 0)
    first_block = sub < 4
    last_block = sub >= s.slots - 4
    first_chunk = sub % 4 == 0
    last_chunk = sub % 4 == 3

    def below_x(v):
        return jnp.where(first_block, 0.0, roll(v, 4, 0))

    def above_x(v):
        return jnp.where(last_block, 0.0, roll(v, -4, 0))

    def below_y(v):
        return jnp.where(first_chunk, 0.0, roll(v, 1, 0))

    def above_y(v):
        return jnp.where(last_chunk, 0.0, roll(v, -1, 0))

    return below_x, above_x, below_y, above_y


def triple(v, low, high):
    n = len(v)
    out = []
    for i in range(0, n, 2):
        pair = v[i] + v[i + 1]
        out.append(pair + (low if i == 0 else v[i - 1]))
        out.append(pair + (high if i + 2 == n else v[i + 2]))
    return out


def plain_triple(v):
    n = len(v)
    out = []
    for i in range(n):
        total = v[i]
        if i > 0:
            total = total + v[i - 1]
        if i + 1 < n:
            total = total + v[i + 1]
        out.append(total)
    return out


def fine_block_sum(s, source, temp, consume):
    below_x, above_x, below_y, above_y = fine_tools(s)
    for par in range(2):
        for yi in range(s.half):
            v = [source[par, xi * s.half + yi] for xi in range(s.bx)]
            for xi, t in enumerate(triple(v, below_x(v[-1]), above_x(v[0]))):
                temp[par, xi * s.half + yi] = t
    for i in range(s.bx // 2):
        sums = []
        for k in range(2):
            xi = 2 * i + k
            both = []
            for par in range(2):
                v = [temp[par, xi * s.half + yi] for yi in range(s.half)]
                both.append(triple(v, below_y(v[-1]), above_y(v[0])))
            even, odd = both
            out_even, out_odd = [], []
            for e, o in zip(even, odd):
                pair = e + o
                out_even.append(pair + roll(o, 1, 1))
                out_odd.append(pair + roll(e, -1, 1))
            sums.append((out_even, out_odd))
        consume(i, sums)


def fine_restrict(s, values, i, store):
    for j in range(s.y1):
        total = None
        for k in range(2):
            for par in range(2):
                for yi in (2 * j, 2 * j + 1):
                    v = values[k][par][yi]
                    total = v if total is None else total + v
        store(i * s.y1 + j, 0.5 * total)


def share_out(s, temp, out, lead):
    count = (s.bx // 2) * s.y1
    for h in range(2):
        for b in range(s.nx):
            out[lead, pl.ds(h * s.rows1 + b * count, count), :] = temp[
                pl.ds(b * 4 + 1 + h, count, stride=s.slots), :
            ]


def split3(v):
    high = v.astype(jnp.bfloat16)
    rest = v - high.astype(f32)
    middle = rest.astype(jnp.bfloat16)
    low = (rest - middle.astype(f32)).astype(jnp.bfloat16)
    return high, middle, low


def exact_dot(v, selection):
    dot = lambda a: jnp.dot(a, selection, preferred_element_type=f32)
    high, middle, low = split3(v)
    return dot(high) + (dot(middle) + dot(low))


def first_kernel(s, place, *refs):
    n = s.nx
    own_g, own_c, x_gc = refs[0], refs[1], refs[2:1 + n]
    refs = refs[1 + n:]
    zside = refs[: 2 * n]
    refs = refs[2 * n:]
    y_a, y_b, g_out, d_out, q_out, share, natural, split_e, split_o, temp, temp1 = refs
    ix, iy, iz = place[0], place[1], place[2]
    even_y = iy % 2 == 0
    even_z = iz % 2 == 0
    L = s.bz
    tile = (s.half, L)
    lane = iota(tile, 1)
    row = iota(tile, 0)
    left = lane < L // 2

    def halo(nextlo, prevhi):
        return (
            jnp.where(left, nextlo, roll(prevhi, L // 2, 1)),
            jnp.where(left, roll(nextlo, L // 2, 1), prevhi),
        )

    for t in range(n):
        base = (ix ^ t) if n & (n - 1) == 0 else (ix + t) % n
        for xi in range(s.bx):
            for ch in range(4):
                if ch in (1, 2):
                    span = pl.ds((ch - 1) * s.half, s.half)
                    if t == 0:
                        g, c = own_g[xi, span, :], own_c[xi, span, :]
                    else:
                        g, c = x_gc[t - 1][0, xi, span, :], x_gc[t - 1][1, xi, span, :]
                    a, b = zside[2 * t][xi, span, :], zside[2 * t + 1][xi, span, :]
                    nextlo = jnp.where(even_z, a, b)
                    prevhi = jnp.where(even_z, b, a)
                    gh, chh = halo(nextlo, prevhi)
                else:
                    use_a = even_y if ch == 3 else jnp.logical_not(even_y)
                    gc = jnp.where(use_a, y_a[t, 0, xi], y_b[t, 0, xi])
                    ab = jnp.where(use_a, y_a[t, 1, xi], y_b[t, 1, xi])
                    turned = roll(gc, HALO, 0)
                    ab_turned = roll(ab, HALO, 0)
                    if ch == 3:
                        keep = row < HALO
                        g, c = gc, turned
                        a, b = ab, ab_turned
                    else:
                        keep = row >= s.half - HALO
                        g, c = turned, gc
                        a, b = ab_turned, ab
                    nextlo = jnp.where(even_z, a, b)
                    prevhi = jnp.where(even_z, b, a)
                    gh, chh = halo(nextlo, prevhi)
                    g, c = jnp.where(keep, g, 0.0), jnp.where(keep, c, 0.0)
                    gh, chh = jnp.where(keep, gh, 0.0), jnp.where(keep, chh, 0.0)
                at = ch * s.rows + xi * s.half
                natural[0, pl.ds(at, s.half), pl.ds(0, L)] = g
                natural[0, pl.ds(at, s.half), pl.ds(L, L)] = gh
                natural[1, pl.ds(at, s.half), pl.ds(0, L)] = c
                natural[1, pl.ds(at, s.half), pl.ds(L, L)] = chh
        source = iota((2 * L, 2 * L), 0)
        target = iota((2 * L, 2 * L), 1)
        wanted = jnp.where(target < L, 2 * target, 2 * (target - L) + 1)
        selection = jnp.where(source == wanted, 1.0, 0.0).astype(jnp.bfloat16)
        start = pl.multiple_of(base * (4 * s.rows), 4 * s.rows)
        for arr in range(2):
            parted = exact_dot(natural[arr], selection)
            split_e[arr, pl.ds(start, 4 * s.rows), :] = parted[:, :L]
            split_o[arr, pl.ds(start, 4 * s.rows), :] = parted[:, L:]

    shape = (s.slots, L)
    subs = iota(shape, 0) % 4
    inside = inside_columns(s, iz, shape) & inside_chunks(s, iy, subs)
    for i in range(s.bx // 2):
        values = []
        for k in range(2):
            both = []
            for par, split in enumerate((split_e, split_o)):
                line = []
                for yi in range(s.half):
                    r = (2 * i + k) * s.half + yi
                    g = split[0, pl.ds(r, s.slots, stride=s.rows), :]
                    c = split[1, pl.ds(r, s.slots, stride=s.rows), :]
                    q = 26.0 + c
                    valid = inside
                    if yi >= HALO:
                        valid = valid & (subs != 3)
                    if yi < s.half - HALO:
                        valid = valid & (subs != 0)
                    d = jnp.where(valid, relaxation / q, 0.0)
                    g_out[par, r] = g
                    q_out[par, r] = q
                    d_out[par, r] = d
                    line.append(c)
                both.append(line)
            values.append(both)

        def keep_c(at, tile1):
            temp1[pl.ds(at * s.slots, s.slots), :] = tile1

        fine_restrict(s, values, i, keep_c)
    share_out(s, temp1, share, 1)
    first_half(s, g_out, d_out, temp, temp1, share, 0)


def first_half(s, g_ref, d_ref, temps, temp1, share, lead):
    e_ref, x_ref = temps.at[0], temps.at[1]
    for par in range(2):
        for r in range(s.rows):
            e_ref[par, r] = d_ref[par, r] * g_ref[par, r]

    def consume(i, sums):
        values = []
        for k in range(2):
            both = []
            for par in range(2):
                line = []
                for yi in range(s.half):
                    r = (2 * i + k) * s.half + yi
                    line.append(
                        (1.0 - relaxation) * g_ref[par, r] - e_ref[par, r] + sums[k][par][yi]
                    )
                both.append(line)
            values.append(both)

        def keep(at, tile1):
            temp1[pl.ds(at * s.slots, s.slots), :] = tile1

        fine_restrict(s, values, i, keep)

    fine_block_sum(s, e_ref, x_ref, consume)
    share_out(s, temp1, share, lead)


def gather_shares(s, iy, shares, lead, spot):
    for t, ref in enumerate(shares):
        at = (iy ^ t) if s.ny & (s.ny - 1) == 0 else (iy + t) % s.ny
        start = pl.multiple_of(at * s.share, s.share)
        spot[pl.ds(start, s.share), :] = ref[lead, pl.ds(0, s.share), :]
    return [spot[pl.ds(r, s.slots1, stride=s.rows1), :] for r in range(s.rows1)]


def middle_sum(s, v, nx, ny, step):
    shape = v[0].shape
    sub = iota(shape, 0)
    first, last = sub == 0, sub == shape[0] - 1
    out = [None] * (nx * ny)
    for yi in range(ny):
        for xi, t in enumerate(plain_triple([v[x * ny + yi] for x in range(nx)])):
            out[xi * ny + yi] = t
    for xi in range(nx):
        line = out[xi * ny:(xi + 1) * ny]
        low = jnp.where(first, 0.0, roll(line[-1], 1, 0))
        high = jnp.where(last, 0.0, roll(line[0], -1, 0))
        out[xi * ny:(xi + 1) * ny] = triple(line, low, high)
    return [t + (roll(t, step, 1) + roll(t, -step, 1)) for t in out]


def middle_restrict(s, v):
    out = []
    for i in range(s.x1 // 2):
        for j in range(s.y1 // 2):
            t = (v[2 * i * s.y1 + 2 * j] + v[2 * i * s.y1 + 2 * j + 1]) + (
                v[(2 * i + 1) * s.y1 + 2 * j] + v[(2 * i + 1) * s.y1 + 2 * j + 1]
            )
            out.append(0.5 * (t + roll(t, -1, 1)))
    return out


def inside_columns(s, iz, shape):
    lanes = iota(shape, 1)
    below = jnp.where(iz < s.nz - 1, 3 * s.bz // 4, s.bz // 2)
    above = jnp.where(iz > 0, 3 * s.bz // 4, s.bz)
    return (lanes < below) | (lanes >= above)


def inside_chunks(s, iy, chunk):
    first = jnp.where(iy > 0, 0, 1)
    last = jnp.where(iy < s.ny - 1, 3, 2)
    return (chunk >= first) & (chunk <= last)


def middle_solve(s, g, d1, d2):
    keep = 1.0 - relaxation
    e0 = [d * t for d, t in zip(d1, g)]
    sums = middle_sum(s, e0, s.x1, s.y1, 1)
    g2 = middle_restrict(s, [keep * t - e + u for t, e, u in zip(g, e0, sums)])
    e = [d * t for d, t in zip(d2, g2)]
    for sweep in range(SWEEPS - 1):
        sums = middle_sum(s, e, s.x1 // 2, s.y1 // 2, 2)
        e = [keep * a + d * ((t - a) + u) for a, d, t, u in zip(e, d2, g2, sums)]
    spread = [a + roll(a, 1, 1) for a in e]
    e1 = [
        e0[x * s.y1 + y] + spread[(x // 2) * (s.y1 // 2) + y // 2]
        for x in range(s.x1)
        for y in range(s.y1)
    ]
    sums = middle_sum(s, e1, s.x1, s.y1, 1)
    return [keep * a + d * ((t - a) + u) for a, d, t, u in zip(e1, d1, g, sums)]


def to_fine(s, iy, e2):
    shape = (s.slots, s.bz)
    sub = iota(shape, 0)
    block = sub // 4
    chunk = sub % 4
    known = inside_chunks(s, iy, chunk)
    out = []
    per = s.bx // 2
    for x in range(per):
        for y in range(s.y1):
            total = jnp.zeros(shape, f32)
            for b in range(s.nx):
                v = e2[(b * per + x) * s.y1 + y]
                shift = (4 * b + 1 - 2 * iy) % s.slots1
                if s.slots1 < s.slots:
                    v = jnp.concatenate([v] * (s.slots // s.slots1), axis=0)
                v = pltpu.roll(v, shift, 0)[: s.slots]
                total = jnp.where(block == b, v, total)
            out.append(jnp.where(known, total, 0.0))
    return out


def second_half(s, g_ref, d_ref, q_ref, coarse, e_ref, x_ref, p_ref, image_store):
    for par in range(2):
        for xi in range(s.bx):
            for yi in range(s.half):
                r = xi * s.half + yi
                e_ref[par, r] = (
                    d_ref[par, r] * g_ref[par, r] + coarse[(xi // 2) * s.y1 + yi // 2]
                )

    def smooth(i, sums):
        for k in range(2):
            for par in range(2):
                for yi in range(s.half):
                    r = (2 * i + k) * s.half + yi
                    e = e_ref[par, r]
                    p_ref[par, r] = (1.0 - relaxation) * e + d_ref[par, r] * (
                        (g_ref[par, r] - e) + sums[k][par][yi]
                    )

    fine_block_sum(s, e_ref, x_ref, smooth)

    def apply(i, sums):
        for k in range(2):
            for par in range(2):
                for yi in range(s.half):
                    r = (2 * i + k) * s.half + yi
                    p = p_ref[par, r]
                    image_store(par, r, (q_ref[par, r] * p + p) - sums[k][par][yi])

    fine_block_sum(s, p_ref, x_ref, apply)


def second_kernel(s, place, *refs):
    shares = refs[: s.ny]
    g_ref, d_ref, q_ref, p_out, image_out, d1_out, d2_out, share = refs[s.ny:s.ny + 8]
    spot, temps, temp1 = refs[s.ny + 8:]
    iy, iz = place[1], place[2]
    g1 = gather_shares(s, iy, shares, 0, spot)
    c1 = gather_shares(s, iy, shares, 1, spot)
    shape = (s.slots1, s.bz)
    inside = inside_columns(s, iz, shape)
    inside2 = inside & (iota(shape, 1) % 2 == 0)
    d1 = [jnp.where(inside, relaxation / (26.0 + c), 0.0) for c in c1]
    d2 = [jnp.where(inside2, relaxation / (26.0 + c), 0.0) for c in middle_restrict(s, c1)]
    for r, d in enumerate(d1):
        d1_out[r] = d
    for r, d in enumerate(d2):
        d2_out[r] = d
    coarse = to_fine(s, iy, middle_solve(s, g1, d1, d2))
    e_ref, x_ref = temps.at[0], temps.at[1]

    def keep(par, r, value):
        image_out[par, r] = value

    second_half(s, g_ref, d_ref, q_ref, coarse, e_ref, x_ref, p_out, keep)
    shape = (s.slots, s.bz)
    chunk = iota(shape, 0) % 4
    own = (iota(shape, 1) < s.bz // 2) & (chunk > 0) & (chunk < 3)
    gammas = [jnp.zeros(shape, f32) for _ in range(4)]
    deltas = [jnp.zeros(shape, f32) for _ in range(4)]
    for par in range(2):
        for r in range(s.rows):
            p = p_out[par, r]
            gammas[r % 4] += g_ref[par, r] * p
            deltas[r % 4] += image_out[par, r] * p
    gamma = jnp.where(own, (gammas[0] + gammas[1]) + (gammas[2] + gammas[3]), 0.0)
    delta = jnp.where(own, (deltas[0] + deltas[1]) + (deltas[2] + deltas[3]), 0.0)
    share[0, pl.ds(s.share, s.slots), :] = gamma
    share[0, pl.ds(s.share + s.slots, s.slots), :] = delta
    first_half(s, image_out, d_ref, temps, temp1, share, 0)


def third_kernel(s, place, *refs):
    shares = refs[: s.ny]
    p_ref, g_ref, d_ref, q_ref, d1_ref, d2_ref = refs[s.ny:s.ny + 6]
    p_out, image_out, mw_out, nw_out = refs[s.ny + 6:s.ny + 10]
    spot, temps, flat, mw_ref = refs[s.ny + 10:]
    ix, iy = place[0], place[1]
    g1 = gather_shares(s, iy, shares, 0, spot)
    d1 = [d1_ref[r] for r in range(s.rows1)]
    d2 = [d2_ref[r] for r in range(s.rows1 // 4)]
    coarse = to_fine(s, iy, middle_solve(s, g1, d1, d2))
    e_ref, x_ref = temps.at[0], temps.at[1]

    def keep(par, r, value):
        flat[par, pl.ds(r * s.slots, s.slots), :] = value

    second_half(s, g_ref, d_ref, q_ref, coarse, e_ref, x_ref, mw_ref, keep)
    L = s.bz
    source = iota((L, L), 0)
    target = iota((L, L), 1)
    wanted = jnp.where(target % 2 == 0, target // 2, L // 2 + target // 2)
    selection = jnp.where(source == wanted, 1.0, 0.0).astype(jnp.bfloat16)
    left = iota((s.half, L), 1) < L // 2
    for ref, out in ((None, nw_out), (mw_ref, mw_out), (g_ref, image_out), (p_ref, p_out)):
        if ref is not None:
            for par in range(2):
                for r in range(s.rows):
                    flat[par, pl.ds(r * s.slots, s.slots), :] = ref[par, r]
        tiles = []
        for xi in range(s.bx):
            for h in range(2):
                at = xi * s.half * s.slots + ix * 4 + 1 + h
                even = flat[0, pl.ds(at, s.half, stride=s.slots), :]
                odd = flat[1, pl.ds(at, s.half, stride=s.slots), :]
                tiles.append(jnp.where(left, even, roll(odd, L // 2, 1)))
        whole = exact_dot(jnp.concatenate(tiles, axis=0), selection)
        for xi in range(s.bx):
            out[xi] = whole[xi * s.by:(xi + 1) * s.by]


def pairs(count):
    return (
        [(i, i ^ 1) for i in range(count) if (i ^ 1) < count],
        [(i, ((i + 1) ^ 1) - 1) for i in range(1, count) if ((i + 1) ^ 1) - 1 < count],
    )


def turns(count):
    if count & (count - 1) == 0:
        return [[(i ^ t, i) for i in range(count)] for t in range(1, count)]
    return [[((i + t) % count, i) for i in range(count)] for t in range(1, count)]


def shards(s, right_side, coefficient):
    L = s.bz
    ix, iy, iz = (lax.axis_index(a) for a in ("gx", "gy", "gz"))
    place = jnp.stack([ix, iy, iz]).astype(jnp.int32)
    smem = pl.BlockSpec(memory_space=pltpu.SMEM)
    vmem = pl.BlockSpec(memory_space=pltpu.VMEM)
    struct = lambda *shape: jax.ShapeDtypeStruct(shape, f32)
    params = pltpu.CompilerParams(vmem_limit_bytes=56 * 2**20)

    low = jnp.concatenate([right_side[:, :, : L // 2], coefficient[:, :, : L // 2]], axis=2)
    high = jnp.concatenate([right_side[:, :, L // 2:], coefficient[:, :, L // 2:]], axis=2)
    even_z = iz % 2 == 0
    send = (jnp.where(even_z, high, low), jnp.where(even_z, low, high))
    both = jnp.stack([right_side, coefficient])
    zpairs = pairs(s.nz)
    zside = [lax.ppermute(v, "gz", p) for v, p in zip(send, zpairs)]
    x_gc = []
    for turn in turns(s.nx):
        x_gc.append(lax.ppermute(both, "gx", turn))
        for v, p in zip(send, zpairs):
            crossed = [
                (a * s.nz + c, b * s.nz + d) for a, b in turn for c, d in p
            ]
            zside.append(lax.ppermute(v, ("gx", "gz"), crossed))

    def edge(rows):
        parts = []
        for t in range(s.nx):
            g, c = (right_side, coefficient) if t == 0 else (x_gc[t - 1][0], x_gc[t - 1][1])
            a, b = zside[2 * t], zside[2 * t + 1]
            parts.append(jnp.concatenate([g[:, rows], c[:, rows]], axis=1))
            parts.append(jnp.concatenate([a[:, rows], b[:, rows]], axis=1))
        return jnp.stack(parts).reshape(s.nx, 2, s.bx, 2 * HALO, L)

    first_rows, last_rows = edge(slice(0, HALO)), edge(slice(s.by - HALO, s.by))
    even_y = iy % 2 == 0
    ypairs = pairs(s.ny)
    y_a = lax.ppermute(jnp.where(even_y, last_rows, first_rows), "gy", ypairs[0])
    y_b = lax.ppermute(jnp.where(even_y, first_rows, last_rows), "gy", ypairs[1])

    fine = struct(2, s.rows, s.slots, L)
    fine_scratch = pltpu.VMEM((2, s.rows, s.slots, L), f32)
    temps = pltpu.VMEM((2, 2, s.rows, s.slots, L), f32)
    temp1 = pltpu.VMEM(((s.bx // 2) * s.y1 * s.slots, L), f32)
    g, d, q, share = pl.pallas_call(
        lambda *refs: first_kernel(s, *refs),
        out_shape=(fine, fine, fine, struct(2, s.share, L)),
        in_specs=[smem] + [vmem] * (2 + (s.nx - 1) + 2 * s.nx + 2),
        out_specs=(vmem,) * 4,
        scratch_shapes=[
            pltpu.VMEM((2, 4 * s.rows, 2 * L), f32),
            pltpu.VMEM((2, s.slots * s.rows, L), f32),
            pltpu.VMEM((2, s.slots * s.rows, L), f32),
            temps,
            temp1,
        ],
        compiler_params=params,
        name="widen",
    )(place, right_side, coefficient, *x_gc, *zside, y_a, y_b)

    spot = pltpu.VMEM((s.slots1 * s.rows1, L), f32)
    yturns = turns(s.ny)
    shares = [share] + [lax.ppermute(share, "gy", turn) for turn in yturns]
    p, image, d1, d2, share = pl.pallas_call(
        lambda *refs: second_kernel(s, *refs),
        out_shape=(
            fine,
            fine,
            struct(s.rows1, s.slots1, L),
            struct(s.rows1 // 4, s.slots1, L),
            struct(1, s.share + 2 * s.slots, L),
        ),
        in_specs=[smem] + [vmem] * (s.ny + 3),
        out_specs=(vmem,) * 5,
        scratch_shapes=[spot, temps, temp1],
        compiler_params=params,
        name="cycle",
    )(place, *shares, g, d, q)

    shares = [share] + [lax.ppermute(share, "gy", turn) for turn in yturns]
    sums = sum(v[0, s.share:] for v in shares)
    sums = sum([lax.ppermute(sums, "gz", turn) for turn in turns(s.nz)], sums)
    nat = struct(s.bx, s.by, L)
    p, image, mw, nw = pl.pallas_call(
        lambda *refs: third_kernel(s, *refs),
        out_shape=(nat,) * 4,
        in_specs=[smem] + [vmem] * (s.ny + 6),
        out_specs=(vmem,) * 4,
        scratch_shapes=[
            spot,
            temps,
            pltpu.VMEM((2, s.rows * s.slots, L), f32),
            fine_scratch,
        ],
        compiler_params=params,
        name="again",
    )(place, *shares, p, image, d, q, d1, d2)

    alpha = jnp.sum(sums[: s.slots]) / jnp.sum(sums[s.slots:])
    return (alpha * p, right_side - alpha * image, p - alpha * mw, image - alpha * nw)


def solution(mesh):
    spec = P("gx", "gy", "gz")
    count = [mesh.shape[a] for a in ("gx", "gy", "gz")]

    def body(right_side, coefficient):
        s = Shape(*count, right_side.shape)
        assert s.bx % 4 == 0 and s.by % 16 == 0 and s.bz % 128 == 0
        return shards(s, right_side, coefficient)

    return jax.shard_map(
        body, mesh=mesh, in_specs=(spec, spec), out_specs=(spec,) * 4, check_vma=False
    )
```

```python
import jax
import jax.numpy as jnp
from jax import lax
from jax.experimental import pallas as pl
from jax.experimental.pallas import tpu as pltpu
from jax.sharding import PartitionSpec as P

SWEEPS = 4
relaxation = 0.6
f32 = jnp.float32

HALO = 4


def roll(value, shift, axis):
    return pltpu.roll(value, shift % value.shape[axis], axis)


def iota(shape, axis):
    return lax.broadcasted_iota(jnp.int32, shape, axis)


class Shape:
    def __init__(self, nx, ny, nz, block):
        self.nx, self.ny, self.nz = nx, ny, nz
        self.bx, self.by, self.bz = block
        self.half = self.by // 2
        self.slots = nx * 4
        self.rows = self.bx * self.half
        self.x1 = nx * self.bx // 2
        self.y1 = self.half // 2
        self.slots1 = 2 * ny
        self.rows1 = self.x1 * self.y1
        self.share = 2 * self.rows1


def fine_tools(s):
    shape = (s.slots, s.bz)
    sub = iota(shape, 0)
    first_block = sub < 4
    last_block = sub >= s.slots - 4
    first_chunk = sub % 4 == 0
    last_chunk = sub % 4 == 3

    def below_x(v):
        return jnp.where(first_block, 0.0, roll(v, 4, 0))

    def above_x(v):
        return jnp.where(last_block, 0.0, roll(v, -4, 0))

    def below_y(v):
        return jnp.where(first_chunk, 0.0, roll(v, 1, 0))

    def above_y(v):
        return jnp.where(last_chunk, 0.0, roll(v, -1, 0))

    return below_x, above_x, below_y, above_y


def triple(v, low, high):
    n = len(v)
    out = []
    for i in range(0, n, 2):
        pair = v[i] + v[i + 1]
        out.append(pair + (low if i == 0 else v[i - 1]))
        out.append(pair + (high if i + 2 == n else v[i + 2]))
    return out


def plain_triple(v):
    n = len(v)
    out = []
    for i in range(n):
        total = v[i]
        if i > 0:
            total = total + v[i - 1]
        if i + 1 < n:
            total = total + v[i + 1]
        out.append(total)
    return out


def fine_block_sum(s, source, temp, consume):
    below_x, above_x, below_y, above_y = fine_tools(s)
    for par in range(2):
        for yi in range(s.half):
            v = [source[par, xi * s.half + yi] for xi in range(s.bx)]
            for xi, t in enumerate(triple(v, below_x(v[-1]), above_x(v[0]))):
                temp[par, xi * s.half + yi] = t
    for i in range(s.bx // 2):
        sums = []
        for k in range(2):
            xi = 2 * i + k
            both = []
            for par in range(2):
                v = [temp[par, xi * s.half + yi] for yi in range(s.half)]
                both.append(triple(v, below_y(v[-1]), above_y(v[0])))
            even, odd = both
            out_even, out_odd = [], []
            for e, o in zip(even, odd):
                pair = e + o
                out_even.append(pair + roll(o, 1, 1))
                out_odd.append(pair + roll(e, -1, 1))
            sums.append((out_even, out_odd))
        consume(i, sums)


def fine_restrict(s, values, i, store):
    for j in range(s.y1):
        total = None
        for k in range(2):
            for par in range(2):
                for yi in (2 * j, 2 * j + 1):
                    v = values[k][par][yi]
                    total = v if total is None else total + v
        store(i * s.y1 + j, 0.5 * total)


def share_out(s, temp, out, lead):
    count = (s.bx // 2) * s.y1
    for h in range(2):
        for b in range(s.nx):
            out[lead, pl.ds(h * s.rows1 + b * count, count), :] = temp[
                pl.ds(b * 4 + 1 + h, count, stride=s.slots), :
            ]


def split3(v):
    high = v.astype(jnp.bfloat16)
    rest = v - high.astype(f32)
    middle = rest.astype(jnp.bfloat16)
    low = (rest - middle.astype(f32)).astype(jnp.bfloat16)
    return high, middle, low


def exact_dot(v, selection):
    dot = lambda a: jnp.dot(a, selection, preferred_element_type=f32)
    high, middle, low = split3(v)
    return dot(high) + (dot(middle) + dot(low))


def first_kernel(s, place, *refs):
    n = s.nx
    own_g, own_c, x_gc = refs[0], refs[1], refs[2:1 + n]
    refs = refs[1 + n:]
    zside = refs[: 2 * n]
    refs = refs[2 * n:]
    y_a, y_b, g_out, d_out, q_out, share, natural, split_e, split_o, temp, temp1 = refs
    ix, iy, iz = place[0], place[1], place[2]
    even_y = iy % 2 == 0
    even_z = iz % 2 == 0
    L = s.bz
    tile = (s.half, L)
    lane = iota(tile, 1)
    row = iota(tile, 0)
    left = lane < L // 2

    def halo(nextlo, prevhi):
        return (
            jnp.where(left, nextlo, roll(prevhi, L // 2, 1)),
            jnp.where(left, roll(nextlo, L // 2, 1), prevhi),
        )

    for t in range(n):
        base = (ix ^ t) if n & (n - 1) == 0 else (ix + t) % n
        for xi in range(s.bx):
            for ch in range(4):
                if ch in (1, 2):
                    span = pl.ds((ch - 1) * s.half, s.half)
                    if t == 0:
                        g, c = own_g[xi, span, :], own_c[xi, span, :]
                    else:
                        g, c = x_gc[t - 1][0, xi, span, :], x_gc[t - 1][1, xi, span, :]
                    a, b = zside[2 * t][xi, span, :], zside[2 * t + 1][xi, span, :]
                    nextlo = jnp.where(even_z, a, b)
                    prevhi = jnp.where(even_z, b, a)
                    gh, chh = halo(nextlo, prevhi)
                else:
                    use_a = even_y if ch == 3 else jnp.logical_not(even_y)
                    gc = jnp.where(use_a, y_a[t, 0, xi], y_b[t, 0, xi])
                    ab = jnp.where(use_a, y_a[t, 1, xi], y_b[t, 1, xi])
                    turned = roll(gc, HALO, 0)
                    ab_turned = roll(ab, HALO, 0)
                    if ch == 3:
                        keep = row < HALO
                        g, c = gc, turned
                        a, b = ab, ab_turned
                    else:
                        keep = row >= s.half - HALO
                        g, c = turned, gc
                        a, b = ab_turned, ab
                    nextlo = jnp.where(even_z, a, b)
                    prevhi = jnp.where(even_z, b, a)
                    gh, chh = halo(nextlo, prevhi)
                    g, c = jnp.where(keep, g, 0.0), jnp.where(keep, c, 0.0)
                    gh, chh = jnp.where(keep, gh, 0.0), jnp.where(keep, chh, 0.0)
                at = ch * s.rows + xi * s.half
                natural[0, pl.ds(at, s.half), pl.ds(0, L)] = g
                natural[0, pl.ds(at, s.half), pl.ds(L, L)] = gh
                natural[1, pl.ds(at, s.half), pl.ds(0, L)] = c
                natural[1, pl.ds(at, s.half), pl.ds(L, L)] = chh
        source = iota((2 * L, 2 * L), 0)
        target = iota((2 * L, 2 * L), 1)
        wanted = jnp.where(target < L, 2 * target, 2 * (target - L) + 1)
        selection = jnp.where(source == wanted, 1.0, 0.0).astype(jnp.bfloat16)
        start = pl.multiple_of(base * (4 * s.rows), 4 * s.rows)
        for arr in range(2):
            parted = exact_dot(natural[arr], selection)
            split_e[arr, pl.ds(start, 4 * s.rows), :] = parted[:, :L]
            split_o[arr, pl.ds(start, 4 * s.rows), :] = parted[:, L:]

    shape = (s.slots, L)
    subs = iota(shape, 0) % 4
    inside = inside_columns(s, iz, shape) & inside_chunks(s, iy, subs)
    for i in range(s.bx // 2):
        values = []
        for k in range(2):
            both = []
            for par, split in enumerate((split_e, split_o)):
                line = []
                for yi in range(s.half):
                    r = (2 * i + k) * s.half + yi
                    g = split[0, pl.ds(r, s.slots, stride=s.rows), :]
                    c = split[1, pl.ds(r, s.slots, stride=s.rows), :]
                    q = 26.0 + c
                    valid = inside
                    if yi >= HALO:
                        valid = valid & (subs != 3)
                    if yi < s.half - HALO:
                        valid = valid & (subs != 0)
                    d = jnp.where(valid, relaxation / q, 0.0)
                    g_out[par, r] = g
                    q_out[par, r] = q
                    d_out[par, r] = d
                    line.append(c)
                both.append(line)
            values.append(both)

        def keep_c(at, tile1):
            temp1[pl.ds(at * s.slots, s.slots), :] = tile1

        fine_restrict(s, values, i, keep_c)
    share_out(s, temp1, share, 1)
    first_half(s, g_out, d_out, temp, temp1, share, 0)


def first_half(s, g_ref, d_ref, temps, temp1, share, lead):
    e_ref, x_ref = temps.at[0], temps.at[1]
    for par in range(2):
        for r in range(s.rows):
            e_ref[par, r] = d_ref[par, r] * g_ref[par, r]

    def consume(i, sums):
        values = []
        for k in range(2):
            both = []
            for par in range(2):
                line = []
                for yi in range(s.half):
                    r = (2 * i + k) * s.half + yi
                    line.append(
                        (1.0 - relaxation) * g_ref[par, r] - e_ref[par, r] + sums[k][par][yi]
                    )
                both.append(line)
            values.append(both)

        def keep(at, tile1):
            temp1[pl.ds(at * s.slots, s.slots), :] = tile1

        fine_restrict(s, values, i, keep)

    fine_block_sum(s, e_ref, x_ref, consume)
    share_out(s, temp1, share, lead)


def gather_shares(s, iy, shares, lead, spot):
    for t, ref in enumerate(shares):
        at = (iy ^ t) if s.ny & (s.ny - 1) == 0 else (iy + t) % s.ny
        start = pl.multiple_of(at * s.share, s.share)
        spot[pl.ds(start, s.share), :] = ref[lead, pl.ds(0, s.share), :]
    return [spot[pl.ds(r, s.slots1, stride=s.rows1), :] for r in range(s.rows1)]


def middle_sum(s, v, nx, ny, step):
    shape = v[0].shape
    sub = iota(shape, 0)
    first, last = sub == 0, sub == shape[0] - 1
    out = [None] * (nx * ny)
    for yi in range(ny):
        for xi, t in enumerate(plain_triple([v[x * ny + yi] for x in range(nx)])):
            out[xi * ny + yi] = t
    for xi in range(nx):
        line = out[xi * ny:(xi + 1) * ny]
        low = jnp.where(first, 0.0, roll(line[-1], 1, 0))
        high = jnp.where(last, 0.0, roll(line[0], -1, 0))
        out[xi * ny:(xi + 1) * ny] = triple(line, low, high)
    return [t + (roll(t, step, 1) + roll(t, -step, 1)) for t in out]


def middle_restrict(s, v):
    out = []
    for i in range(s.x1 // 2):
        for j in range(s.y1 // 2):
            t = (v[2 * i * s.y1 + 2 * j] + v[2 * i * s.y1 + 2 * j + 1]) + (
                v[(2 * i + 1) * s.y1 + 2 * j] + v[(2 * i + 1) * s.y1 + 2 * j + 1]
            )
            out.append(0.5 * (t + roll(t, -1, 1)))
    return out


def inside_columns(s, iz, shape):
    lanes = iota(shape, 1)
    below = jnp.where(iz < s.nz - 1, 3 * s.bz // 4, s.bz // 2)
    above = jnp.where(iz > 0, 3 * s.bz // 4, s.bz)
    return (lanes < below) | (lanes >= above)


def inside_chunks(s, iy, chunk):
    first = jnp.where(iy > 0, 0, 1)
    last = jnp.where(iy < s.ny - 1, 3, 2)
    return (chunk >= first) & (chunk <= last)


def middle_solve(s, g, d1, d2):
    keep = 1.0 - relaxation
    e0 = [d * t for d, t in zip(d1, g)]
    sums = middle_sum(s, e0, s.x1, s.y1, 1)
    g2 = middle_restrict(s, [keep * t - e + u for t, e, u in zip(g, e0, sums)])
    e = [d * t for d, t in zip(d2, g2)]
    for sweep in range(SWEEPS - 1):
        sums = middle_sum(s, e, s.x1 // 2, s.y1 // 2, 2)
        e = [keep * a + d * ((t - a) + u) for a, d, t, u in zip(e, d2, g2, sums)]
    spread = [a + roll(a, 1, 1) for a in e]
    e1 = [
        e0[x * s.y1 + y] + spread[(x // 2) * (s.y1 // 2) + y // 2]
        for x in range(s.x1)
        for y in range(s.y1)
    ]
    sums = middle_sum(s, e1, s.x1, s.y1, 1)
    return [keep * a + d * ((t - a) + u) for a, d, t, u in zip(e1, d1, g, sums)]


def to_fine(s, iy, e2):
    shape = (s.slots, s.bz)
    sub = iota(shape, 0)
    block = sub // 4
    chunk = sub % 4
    known = inside_chunks(s, iy, chunk)
    out = []
    per = s.bx // 2
    for x in range(per):
        for y in range(s.y1):
            total = jnp.zeros(shape, f32)
            for b in range(s.nx):
                v = e2[(b * per + x) * s.y1 + y]
                shift = (4 * b + 1 - 2 * iy) % s.slots1
                if s.slots1 < s.slots:
                    v = jnp.concatenate([v] * (s.slots // s.slots1), axis=0)
                v = pltpu.roll(v, shift, 0)[: s.slots]
                total = jnp.where(block == b, v, total)
            out.append(jnp.where(known, total, 0.0))
    return out


def second_half(s, g_ref, d_ref, q_ref, coarse, e_ref, x_ref, p_ref, image_store):
    for par in range(2):
        for xi in range(s.bx):
            for yi in range(s.half):
                r = xi * s.half + yi
                e_ref[par, r] = (
                    d_ref[par, r] * g_ref[par, r] + coarse[(xi // 2) * s.y1 + yi // 2]
                )

    def smooth(i, sums):
        for k in range(2):
            for par in range(2):
                for yi in range(s.half):
                    r = (2 * i + k) * s.half + yi
                    e = e_ref[par, r]
                    p_ref[par, r] = (1.0 - relaxation) * e + d_ref[par, r] * (
                        (g_ref[par, r] - e) + sums[k][par][yi]
                    )

    fine_block_sum(s, e_ref, x_ref, smooth)

    def apply(i, sums):
        for k in range(2):
            for par in range(2):
                for yi in range(s.half):
                    r = (2 * i + k) * s.half + yi
                    p = p_ref[par, r]
                    image_store(par, r, (q_ref[par, r] * p + p) - sums[k][par][yi])

    fine_block_sum(s, p_ref, x_ref, apply)


def second_kernel(s, place, *refs):
    shares = refs[: s.ny]
    g_ref, d_ref, q_ref, p_out, image_out, d1_out, d2_out, share = refs[s.ny:s.ny + 8]
    spot, temps, temp1 = refs[s.ny + 8:]
    iy, iz = place[1], place[2]
    g1 = gather_shares(s, iy, shares, 0, spot)
    c1 = gather_shares(s, iy, shares, 1, spot)
    shape = (s.slots1, s.bz)
    inside = inside_columns(s, iz, shape)
    inside2 = inside & (iota(shape, 1) % 2 == 0)
    d1 = [jnp.where(inside, relaxation / (26.0 + c), 0.0) for c in c1]
    d2 = [jnp.where(inside2, relaxation / (26.0 + c), 0.0) for c in middle_restrict(s, c1)]
    for r, d in enumerate(d1):
        d1_out[r] = d
    for r, d in enumerate(d2):
        d2_out[r] = d
    coarse = to_fine(s, iy, middle_solve(s, g1, d1, d2))
    e_ref, x_ref = temps.at[0], temps.at[1]

    def keep(par, r, value):
        image_out[par, r] = value

    second_half(s, g_ref, d_ref, q_ref, coarse, e_ref, x_ref, p_out, keep)
    shape = (s.slots, s.bz)
    chunk = iota(shape, 0) % 4
    own = (iota(shape, 1) < s.bz // 2) & (chunk > 0) & (chunk < 3)
    gammas = [jnp.zeros(shape, f32) for _ in range(4)]
    deltas = [jnp.zeros(shape, f32) for _ in range(4)]
    for par in range(2):
        for r in range(s.rows):
            p = p_out[par, r]
            gammas[r % 4] += g_ref[par, r] * p
            deltas[r % 4] += image_out[par, r] * p
    gamma = jnp.where(own, (gammas[0] + gammas[1]) + (gammas[2] + gammas[3]), 0.0)
    delta = jnp.where(own, (deltas[0] + deltas[1]) + (deltas[2] + deltas[3]), 0.0)
    share[0, pl.ds(s.share, s.slots), :] = gamma
    share[0, pl.ds(s.share + s.slots, s.slots), :] = delta
    first_half(s, image_out, d_ref, temps, temp1, share, 0)


def third_kernel(s, place, *refs):
    shares = refs[: s.ny]
    sums = refs[s.ny:s.ny + s.nz]
    refs = refs[s.ny + s.nz:]
    right, p_ref, g_ref, d_ref, q_ref, d1_ref, d2_ref = refs[:7]
    outs = refs[7:11]
    spot, temps, flat, mw_ref = refs[11:]
    ix, iy = place[0], place[1]
    g1 = gather_shares(s, iy, shares, 0, spot)
    d1 = [d1_ref[r] for r in range(s.rows1)]
    d2 = [d2_ref[r] for r in range(s.rows1 // 4)]
    coarse = to_fine(s, iy, middle_solve(s, g1, d1, d2))
    e_ref, x_ref = temps.at[0], temps.at[1]

    def keep(par, r, value):
        flat[par, pl.ds(r * s.slots, s.slots), :] = value

    second_half(s, g_ref, d_ref, q_ref, coarse, e_ref, x_ref, mw_ref, keep)
    L = s.bz
    source = iota((L, L), 0)
    target = iota((L, L), 1)
    wanted = jnp.where(target % 2 == 0, target // 2, L // 2 + target // 2)
    selection = jnp.where(source == wanted, 1.0, 0.0).astype(jnp.bfloat16)
    left = iota((s.half, L), 1) < L // 2
    total = sums[0][...]
    for v in sums[1:]:
        total = total + v[...]
    gamma = jnp.sum(total[: s.slots], keepdims=True)
    delta = jnp.sum(total[s.slots:], keepdims=True)
    alpha = gamma / delta
    natural = []
    for ref in (None, mw_ref, g_ref, p_ref):
        if ref is not None:
            for par in range(2):
                for r in range(s.rows):
                    flat[par, pl.ds(r * s.slots, s.slots), :] = ref[par, r]
        tiles = []
        for xi in range(s.bx):
            for h in range(2):
                at = xi * s.half * s.slots + ix * 4 + 1 + h
                even = flat[0, pl.ds(at, s.half, stride=s.slots), :]
                odd = flat[1, pl.ds(at, s.half, stride=s.slots), :]
                tiles.append(jnp.where(left, even, roll(odd, L // 2, 1)))
        natural.append(exact_dot(jnp.concatenate(tiles, axis=0), selection))
    nw, mw, image, p = natural
    for xi in range(s.bx):
        at = slice(xi * s.by, (xi + 1) * s.by)
        outs[0][xi] = alpha * p[at]
        outs[1][xi] = right[xi] - alpha * image[at]
        outs[2][xi] = p[at] - alpha * mw[at]
        outs[3][xi] = image[at] - alpha * nw[at]


def pairs(count):
    return (
        [(i, i ^ 1) for i in range(count) if (i ^ 1) < count],
        [(i, ((i + 1) ^ 1) - 1) for i in range(1, count) if ((i + 1) ^ 1) - 1 < count],
    )


def turns(count):
    if count & (count - 1) == 0:
        return [[(i ^ t, i) for i in range(count)] for t in range(1, count)]
    return [[((i + t) % count, i) for i in range(count)] for t in range(1, count)]


def shards(s, right_side, coefficient):
    L = s.bz
    ix, iy, iz = (lax.axis_index(a) for a in ("gx", "gy", "gz"))
    place = jnp.stack([ix, iy, iz]).astype(jnp.int32)
    smem = pl.BlockSpec(memory_space=pltpu.SMEM)
    vmem = pl.BlockSpec(memory_space=pltpu.VMEM)
    struct = lambda *shape: jax.ShapeDtypeStruct(shape, f32)
    params = pltpu.CompilerParams(vmem_limit_bytes=16 * 4 * 2 * s.rows * s.slots * L)

    low = jnp.concatenate([right_side[:, :, : L // 2], coefficient[:, :, : L // 2]], axis=2)
    high = jnp.concatenate([right_side[:, :, L // 2:], coefficient[:, :, L // 2:]], axis=2)
    even_z = iz % 2 == 0
    send = (jnp.where(even_z, high, low), jnp.where(even_z, low, high))
    both = jnp.stack([right_side, coefficient])
    zpairs = pairs(s.nz)
    zside = [lax.ppermute(v, "gz", p) for v, p in zip(send, zpairs)]
    x_gc = []
    for turn in turns(s.nx):
        x_gc.append(lax.ppermute(both, "gx", turn))
        for v, p in zip(send, zpairs):
            crossed = [
                (a * s.nz + c, b * s.nz + d) for a, b in turn for c, d in p
            ]
            zside.append(lax.ppermute(v, ("gx", "gz"), crossed))

    def edge(rows):
        parts = []
        for t in range(s.nx):
            g, c = (right_side, coefficient) if t == 0 else (x_gc[t - 1][0], x_gc[t - 1][1])
            a, b = zside[2 * t], zside[2 * t + 1]
            parts.append(jnp.concatenate([g[:, rows], c[:, rows]], axis=1))
            parts.append(jnp.concatenate([a[:, rows], b[:, rows]], axis=1))
        return jnp.stack(parts).reshape(s.nx, 2, s.bx, 2 * HALO, L)

    first_rows, last_rows = edge(slice(0, HALO)), edge(slice(s.by - HALO, s.by))
    even_y = iy % 2 == 0
    ypairs = pairs(s.ny)
    y_a = lax.ppermute(jnp.where(even_y, last_rows, first_rows), "gy", ypairs[0])
    y_b = lax.ppermute(jnp.where(even_y, first_rows, last_rows), "gy", ypairs[1])

    fine = struct(2, s.rows, s.slots, L)
    fine_scratch = pltpu.VMEM((2, s.rows, s.slots, L), f32)
    temps = pltpu.VMEM((2, 2, s.rows, s.slots, L), f32)
    temp1 = pltpu.VMEM(((s.bx // 2) * s.y1 * s.slots, L), f32)
    g, d, q, share = pl.pallas_call(
        lambda *refs: first_kernel(s, *refs),
        out_shape=(fine, fine, fine, struct(2, s.share, L)),
        in_specs=[smem] + [vmem] * (2 + (s.nx - 1) + 2 * s.nx + 2),
        out_specs=(vmem,) * 4,
        scratch_shapes=[
            pltpu.VMEM((2, 4 * s.rows, 2 * L), f32),
            pltpu.VMEM((2, s.slots * s.rows, L), f32),
            pltpu.VMEM((2, s.slots * s.rows, L), f32),
            temps,
            temp1,
        ],
        compiler_params=params,
        name="widen",
    )(place, right_side, coefficient, *x_gc, *zside, y_a, y_b)

    spot = pltpu.VMEM((s.slots1 * s.rows1, L), f32)
    yturns = turns(s.ny)
    shares = [share] + [lax.ppermute(share, "gy", turn) for turn in yturns]
    p, image, d1, d2, share = pl.pallas_call(
        lambda *refs: second_kernel(s, *refs),
        out_shape=(
            fine,
            fine,
            struct(s.rows1, s.slots1, L),
            struct(s.rows1 // 4, s.slots1, L),
            struct(1, s.share + 2 * s.slots, L),
        ),
        in_specs=[smem] + [vmem] * (s.ny + 3),
        out_specs=(vmem,) * 5,
        scratch_shapes=[spot, temps, temp1],
        compiler_params=params,
        name="cycle",
    )(place, *shares, g, d, q)

    shares = [share] + [lax.ppermute(share, "gy", turn) for turn in yturns]
    sums = sum(v[0, s.share:] for v in shares)
    sums = [sums] + [lax.ppermute(sums, "gz", turn) for turn in turns(s.nz)]
    return pl.pallas_call(
        lambda *refs: third_kernel(s, *refs),
        out_shape=(struct(s.bx, s.by, L),) * 4,
        in_specs=[smem] + [vmem] * (s.ny + s.nz + 7),
        out_specs=(vmem,) * 4,
        scratch_shapes=[
            spot,
            temps,
            pltpu.VMEM((2, s.rows * s.slots, L), f32),
            fine_scratch,
        ],
        compiler_params=params,
        name="again",
    )(place, *shares, *sums, right_side, p, image, d, q, d1, d2)


def solution(mesh):
    spec = P("gx", "gy", "gz")
    count = [mesh.shape[a] for a in ("gx", "gy", "gz")]

    def body(right_side, coefficient):
        s = Shape(*count, right_side.shape)
        assert s.bx % 4 == 0 and s.by % 16 == 0 and s.bz % 128 == 0
        return shards(s, right_side, coefficient)

    return jax.shard_map(
        body, mesh=mesh, in_specs=(spec, spec), out_specs=(spec,) * 4, check_vma=False
    )
```

```python
import jax
import jax.numpy as jnp
from jax import lax
from jax.experimental import pallas as pl
from jax.experimental.pallas import tpu as pltpu
from jax.sharding import PartitionSpec as P

SWEEPS = 4
relaxation = 0.6
f32 = jnp.float32

HALO = 4


def roll(value, shift, axis):
    return pltpu.roll(value, shift % value.shape[axis], axis)


def position():
    return tuple(lax.axis_index(a) for a in ("gx", "gy", "gz"))


def iota(shape, axis):
    return lax.broadcasted_iota(jnp.int32, shape, axis)


class Shape:
    def __init__(self, nx, ny, nz, block):
        self.nx, self.ny, self.nz = nx, ny, nz
        self.bx, self.by, self.bz = block
        self.half = self.by // 2
        self.slots = nx * 4
        self.rows = self.bx * self.half
        self.x1 = nx * self.bx // 2
        self.y1 = self.half // 2
        self.slots1 = 2 * ny
        self.rows1 = self.x1 * self.y1
        self.share = 2 * self.rows1


def fine_tools(s):
    shape = (s.slots, s.bz)
    sub = iota(shape, 0)
    first_block = sub < 4
    last_block = sub >= s.slots - 4
    first_chunk = sub % 4 == 0
    last_chunk = sub % 4 == 3

    def below_x(v):
        return jnp.where(first_block, 0.0, roll(v, 4, 0))

    def above_x(v):
        return jnp.where(last_block, 0.0, roll(v, -4, 0))

    def below_y(v):
        return jnp.where(first_chunk, 0.0, roll(v, 1, 0))

    def above_y(v):
        return jnp.where(last_chunk, 0.0, roll(v, -1, 0))

    return below_x, above_x, below_y, above_y


def triple(v, low, high):
    n = len(v)
    out = []
    for i in range(0, n, 2):
        pair = v[i] + v[i + 1]
        out.append(pair + (low if i == 0 else v[i - 1]))
        out.append(pair + (high if i + 2 == n else v[i + 2]))
    return out


def plain_triple(v):
    n = len(v)
    out = []
    for i in range(n):
        total = v[i]
        if i > 0:
            total = total + v[i - 1]
        if i + 1 < n:
            total = total + v[i + 1]
        out.append(total)
    return out


def fine_block_sum(s, source, temp, consume):
    below_x, above_x, below_y, above_y = fine_tools(s)
    for par in range(2):
        for yi in range(s.half):
            v = [source[par, xi * s.half + yi] for xi in range(s.bx)]
            for xi, t in enumerate(triple(v, below_x(v[-1]), above_x(v[0]))):
                temp[par, xi * s.half + yi] = t
    for i in range(s.bx // 2):
        sums = []
        for k in range(2):
            xi = 2 * i + k
            both = []
            for par in range(2):
                v = [temp[par, xi * s.half + yi] for yi in range(s.half)]
                both.append(triple(v, below_y(v[-1]), above_y(v[0])))
            even, odd = both
            out_even, out_odd = [], []
            for e, o in zip(even, odd):
                pair = e + o
                out_even.append(pair + roll(o, 1, 1))
                out_odd.append(pair + roll(e, -1, 1))
            sums.append((out_even, out_odd))
        consume(i, sums)


def fine_restrict(s, values, i, store):
    for j in range(s.y1):
        total = None
        for k in range(2):
            for par in range(2):
                for yi in (2 * j, 2 * j + 1):
                    v = values[k][par][yi]
                    total = v if total is None else total + v
        store(i * s.y1 + j, 0.5 * total)


def share_out(s, temp, out, lead):
    count = (s.bx // 2) * s.y1
    for h in range(2):
        for b in range(s.nx):
            out[lead, pl.ds(h * s.rows1 + b * count, count), :] = temp[
                pl.ds(b * 4 + 1 + h, count, stride=s.slots), :
            ]


def split3(v):
    high = v.astype(jnp.bfloat16)
    rest = v - high.astype(f32)
    middle = rest.astype(jnp.bfloat16)
    low = (rest - middle.astype(f32)).astype(jnp.bfloat16)
    return high, middle, low


def exact_dot(v, selection):
    dot = lambda a: jnp.dot(a, selection, preferred_element_type=f32)
    high, middle, low = split3(v)
    return dot(high) + (dot(middle) + dot(low))


def first_kernel(s, *refs):
    n = s.nx
    own_g, own_c, x_gc = refs[0], refs[1], refs[2:1 + n]
    refs = refs[1 + n:]
    zside = refs[:n]
    refs = refs[n:]
    y_a, y_b, g_out, d_out, q_out, share, natural, split_e, split_o, temp, temp1 = refs
    ix, iy, iz = position()
    even_y = iy % 2 == 0
    even_z = iz % 2 == 0
    L = s.bz
    tile = (s.half, L)
    lane = iota(tile, 1)
    row = iota(tile, 0)
    left = lane < L // 2

    def halo(nextlo, prevhi):
        return (
            jnp.where(left, nextlo, roll(prevhi, L // 2, 1)),
            jnp.where(left, roll(nextlo, L // 2, 1), prevhi),
        )

    for t in range(n):
        base = (ix ^ t) if n & (n - 1) == 0 else (ix + t) % n
        for xi in range(s.bx):
            for ch in range(4):
                if ch in (1, 2):
                    span = pl.ds((ch - 1) * s.half, s.half)
                    if t == 0:
                        g, c = own_g[xi, span, :], own_c[xi, span, :]
                    else:
                        g, c = x_gc[t - 1][0, xi, span, :], x_gc[t - 1][1, xi, span, :]
                    a, b = zside[t][0, xi, span, :], zside[t][1, xi, span, :]
                    nextlo = jnp.where(even_z, a, b)
                    prevhi = jnp.where(even_z, b, a)
                    gh, chh = halo(nextlo, prevhi)
                else:
                    use_a = even_y if ch == 3 else jnp.logical_not(even_y)
                    gc = jnp.where(use_a, y_a[t, 0, xi], y_b[t, 0, xi])
                    ab = jnp.where(use_a, y_a[t, 1, xi], y_b[t, 1, xi])
                    turned = roll(gc, HALO, 0)
                    ab_turned = roll(ab, HALO, 0)
                    if ch == 3:
                        keep = row < HALO
                        g, c = gc, turned
                        a, b = ab, ab_turned
                    else:
                        keep = row >= s.half - HALO
                        g, c = turned, gc
                        a, b = ab_turned, ab
                    nextlo = jnp.where(even_z, a, b)
                    prevhi = jnp.where(even_z, b, a)
                    gh, chh = halo(nextlo, prevhi)
                    g, c = jnp.where(keep, g, 0.0), jnp.where(keep, c, 0.0)
                    gh, chh = jnp.where(keep, gh, 0.0), jnp.where(keep, chh, 0.0)
                at = ch * s.rows + xi * s.half
                natural[0, pl.ds(at, s.half), pl.ds(0, L)] = g
                natural[0, pl.ds(at, s.half), pl.ds(L, L)] = gh
                natural[1, pl.ds(at, s.half), pl.ds(0, L)] = c
                natural[1, pl.ds(at, s.half), pl.ds(L, L)] = chh
        source = iota((2 * L, 2 * L), 0)
        target = iota((2 * L, 2 * L), 1)
        wanted = jnp.where(target < L, 2 * target, 2 * (target - L) + 1)
        selection = jnp.where(source == wanted, 1.0, 0.0).astype(jnp.bfloat16)
        start = pl.multiple_of(base * (4 * s.rows), 4 * s.rows)
        for arr in range(2):
            parted = exact_dot(natural[arr], selection)
            split_e[arr, pl.ds(start, 4 * s.rows), :] = parted[:, :L]
            split_o[arr, pl.ds(start, 4 * s.rows), :] = parted[:, L:]

    shape = (s.slots, L)
    subs = iota(shape, 0) % 4
    inside = inside_columns(s, iz, shape) & inside_chunks(s, iy, subs)
    for i in range(s.bx // 2):
        values = []
        for k in range(2):
            both = []
            for par, split in enumerate((split_e, split_o)):
                line = []
                for yi in range(s.half):
                    r = (2 * i + k) * s.half + yi
                    g = split[0, pl.ds(r, s.slots, stride=s.rows), :]
                    c = split[1, pl.ds(r, s.slots, stride=s.rows), :]
                    q = 26.0 + c
                    valid = inside
                    if yi >= HALO:
                        valid = valid & (subs != 3)
                    if yi < s.half - HALO:
                        valid = valid & (subs != 0)
                    d = jnp.where(valid, relaxation / q, 0.0)
                    g_out[par, r] = g
                    q_out[par, r] = q
                    d_out[par, r] = d
                    line.append(c)
                both.append(line)
            values.append(both)

        def keep_c(at, tile1):
            temp1[pl.ds(at * s.slots, s.slots), :] = tile1

        fine_restrict(s, values, i, keep_c)
    share_out(s, temp1, share, 1)
    first_half(s, g_out, d_out, temp, temp1, share, 0)


def first_half(s, g_ref, d_ref, temps, temp1, share, lead):
    e_ref, x_ref = temps.at[0], temps.at[1]
    for par in range(2):
        for r in range(s.rows):
            e_ref[par, r] = d_ref[par, r] * g_ref[par, r]

    def consume(i, sums):
        values = []
        for k in range(2):
            both = []
            for par in range(2):
                line = []
                for yi in range(s.half):
                    r = (2 * i + k) * s.half + yi
                    line.append(
                        (1.0 - relaxation) * g_ref[par, r] - e_ref[par, r] + sums[k][par][yi]
                    )
                both.append(line)
            values.append(both)

        def keep(at, tile1):
            temp1[pl.ds(at * s.slots, s.slots), :] = tile1

        fine_restrict(s, values, i, keep)

    fine_block_sum(s, e_ref, x_ref, consume)
    share_out(s, temp1, share, lead)


def gather_shares(s, iy, shares, lead, spot):
    for t, ref in enumerate(shares):
        at = (iy ^ t) if s.ny & (s.ny - 1) == 0 else (iy + t) % s.ny
        start = pl.multiple_of(at * s.share, s.share)
        spot[pl.ds(start, s.share), :] = ref[lead, pl.ds(0, s.share), :]
    return [spot[pl.ds(r, s.slots1, stride=s.rows1), :] for r in range(s.rows1)]


def middle_sum(s, v, nx, ny, step):
    shape = v[0].shape
    sub = iota(shape, 0)
    first, last = sub == 0, sub == shape[0] - 1
    out = [None] * (nx * ny)
    for yi in range(ny):
        for xi, t in enumerate(plain_triple([v[x * ny + yi] for x in range(nx)])):
            out[xi * ny + yi] = t
    for xi in range(nx):
        line = out[xi * ny:(xi + 1) * ny]
        low = jnp.where(first, 0.0, roll(line[-1], 1, 0))
        high = jnp.where(last, 0.0, roll(line[0], -1, 0))
        out[xi * ny:(xi + 1) * ny] = triple(line, low, high)
    return [t + (roll(t, step, 1) + roll(t, -step, 1)) for t in out]


def middle_restrict(s, v):
    out = []
    for i in range(s.x1 // 2):
        for j in range(s.y1 // 2):
            t = (v[2 * i * s.y1 + 2 * j] + v[2 * i * s.y1 + 2 * j + 1]) + (
                v[(2 * i + 1) * s.y1 + 2 * j] + v[(2 * i + 1) * s.y1 + 2 * j + 1]
            )
            out.append(0.5 * (t + roll(t, -1, 1)))
    return out


def inside_columns(s, iz, shape):
    lanes = iota(shape, 1)
    below = jnp.where(iz < s.nz - 1, 3 * s.bz // 4, s.bz // 2)
    above = jnp.where(iz > 0, 3 * s.bz // 4, s.bz)
    return (lanes < below) | (lanes >= above)


def inside_chunks(s, iy, chunk):
    first = jnp.where(iy > 0, 0, 1)
    last = jnp.where(iy < s.ny - 1, 3, 2)
    return (chunk >= first) & (chunk <= last)


def middle_solve(s, g, d1, d2):
    keep = 1.0 - relaxation
    e0 = [d * t for d, t in zip(d1, g)]
    sums = middle_sum(s, e0, s.x1, s.y1, 1)
    g2 = middle_restrict(s, [keep * t - e + u for t, e, u in zip(g, e0, sums)])
    e = [d * t for d, t in zip(d2, g2)]
    for sweep in range(SWEEPS - 1):
        sums = middle_sum(s, e, s.x1 // 2, s.y1 // 2, 2)
        e = [keep * a + d * ((t - a) + u) for a, d, t, u in zip(e, d2, g2, sums)]
    spread = [a + roll(a, 1, 1) for a in e]
    e1 = [
        e0[x * s.y1 + y] + spread[(x // 2) * (s.y1 // 2) + y // 2]
        for x in range(s.x1)
        for y in range(s.y1)
    ]
    sums = middle_sum(s, e1, s.x1, s.y1, 1)
    return [keep * a + d * ((t - a) + u) for a, d, t, u in zip(e1, d1, g, sums)]


def to_fine(s, iy, e2):
    shape = (s.slots, s.bz)
    sub = iota(shape, 0)
    block = sub // 4
    chunk = sub % 4
    known = inside_chunks(s, iy, chunk)
    out = []
    per = s.bx // 2
    for x in range(per):
        for y in range(s.y1):
            total = jnp.zeros(shape, f32)
            for b in range(s.nx):
                v = e2[(b * per + x) * s.y1 + y]
                shift = (4 * b + 1 - 2 * iy) % s.slots1
                if s.slots1 < s.slots:
                    v = jnp.concatenate([v] * (s.slots // s.slots1), axis=0)
                v = pltpu.roll(v, shift, 0)[: s.slots]
                total = jnp.where(block == b, v, total)
            out.append(jnp.where(known, total, 0.0))
    return out


def second_half(s, g_ref, d_ref, q_ref, coarse, e_ref, x_ref, p_ref, image_store):
    for par in range(2):
        for xi in range(s.bx):
            for yi in range(s.half):
                r = xi * s.half + yi
                e_ref[par, r] = (
                    d_ref[par, r] * g_ref[par, r] + coarse[(xi // 2) * s.y1 + yi // 2]
                )

    def smooth(i, sums):
        for k in range(2):
            for par in range(2):
                for yi in range(s.half):
                    r = (2 * i + k) * s.half + yi
                    e = e_ref[par, r]
                    p_ref[par, r] = (1.0 - relaxation) * e + d_ref[par, r] * (
                        (g_ref[par, r] - e) + sums[k][par][yi]
                    )

    fine_block_sum(s, e_ref, x_ref, smooth)

    def apply(i, sums):
        for k in range(2):
            for par in range(2):
                for yi in range(s.half):
                    r = (2 * i + k) * s.half + yi
                    p = p_ref[par, r]
                    image_store(par, r, (q_ref[par, r] * p + p) - sums[k][par][yi])

    fine_block_sum(s, p_ref, x_ref, apply)


def second_kernel(s, *refs):
    shares = refs[: s.ny]
    g_ref, d_ref, q_ref, p_out, image_out, d1_out, d2_out, share = refs[s.ny:s.ny + 8]
    spot, temps, temp1 = refs[s.ny + 8:]
    ix, iy, iz = position()
    g1 = gather_shares(s, iy, shares, 0, spot)
    c1 = gather_shares(s, iy, shares, 1, spot)
    shape = (s.slots1, s.bz)
    inside = inside_columns(s, iz, shape)
    inside2 = inside & (iota(shape, 1) % 2 == 0)
    d1 = [jnp.where(inside, relaxation / (26.0 + c), 0.0) for c in c1]
    d2 = [jnp.where(inside2, relaxation / (26.0 + c), 0.0) for c in middle_restrict(s, c1)]
    for r, d in enumerate(d1):
        d1_out[r] = d
    for r, d in enumerate(d2):
        d2_out[r] = d
    coarse = to_fine(s, iy, middle_solve(s, g1, d1, d2))
    e_ref, x_ref = temps.at[0], temps.at[1]

    def keep(par, r, value):
        image_out[par, r] = value

    second_half(s, g_ref, d_ref, q_ref, coarse, e_ref, x_ref, p_out, keep)
    shape = (s.slots, s.bz)
    chunk = iota(shape, 0) % 4
    own = (iota(shape, 1) < s.bz // 2) & (chunk > 0) & (chunk < 3)
    gammas = [jnp.zeros(shape, f32) for _ in range(4)]
    deltas = [jnp.zeros(shape, f32) for _ in range(4)]
    for par in range(2):
        for r in range(s.rows):
            p = p_out[par, r]
            gammas[r % 4] += g_ref[par, r] * p
            deltas[r % 4] += image_out[par, r] * p
    gamma = jnp.where(own, (gammas[0] + gammas[1]) + (gammas[2] + gammas[3]), 0.0)
    delta = jnp.where(own, (deltas[0] + deltas[1]) + (deltas[2] + deltas[3]), 0.0)
    share[0, pl.ds(s.share, s.slots), :] = gamma
    share[0, pl.ds(s.share + s.slots, s.slots), :] = delta
    first_half(s, image_out, d_ref, temps, temp1, share, 0)


def third_kernel(s, *refs):
    shares = refs[: s.ny]
    p_ref, g_ref, d_ref, q_ref, d1_ref, d2_ref, out = refs[s.ny:s.ny + 7]
    spot, temps, flat, mw_ref = refs[s.ny + 7:]
    ix, iy, iz = position()
    g1 = gather_shares(s, iy, shares, 0, spot)
    d1 = [d1_ref[r] for r in range(s.rows1)]
    d2 = [d2_ref[r] for r in range(s.rows1 // 4)]
    coarse = to_fine(s, iy, middle_solve(s, g1, d1, d2))
    e_ref, x_ref = temps.at[0], temps.at[1]

    def keep(par, r, value):
        flat[par, pl.ds(r * s.slots, s.slots), :] = value

    second_half(s, g_ref, d_ref, q_ref, coarse, e_ref, x_ref, mw_ref, keep)
    L = s.bz
    source = iota((L, L), 0)
    target = iota((L, L), 1)
    wanted = jnp.where(target % 2 == 0, target // 2, L // 2 + target // 2)
    selection = jnp.where(source == wanted, 1.0, 0.0).astype(jnp.bfloat16)
    left = iota((s.half, L), 1) < L // 2
    for k, ref in enumerate((None, mw_ref, g_ref, p_ref)):
        if ref is not None:
            for par in range(2):
                for r in range(s.rows):
                    flat[par, pl.ds(r * s.slots, s.slots), :] = ref[par, r]
        tiles = []
        for xi in range(s.bx):
            for h in range(2):
                at = xi * s.half * s.slots + ix * 4 + 1 + h
                even = flat[0, pl.ds(at, s.half, stride=s.slots), :]
                odd = flat[1, pl.ds(at, s.half, stride=s.slots), :]
                tiles.append(jnp.where(left, even, roll(odd, L // 2, 1)))
        out[k] = exact_dot(jnp.concatenate(tiles, axis=0), selection)


def last_kernel(s, *refs):
    right, natural = refs[s.nz:s.nz + 2]
    outs = refs[s.nz + 2:]
    total = refs[0][...]
    for v in refs[1:s.nz]:
        total = total + v[...]
    gamma = jnp.sum(total[: s.slots], keepdims=True)
    delta = jnp.sum(total[s.slots:], keepdims=True)
    alpha = gamma / delta
    for xi in range(s.bx):
        at = pl.ds(xi * s.by, s.by)
        nw, mw, image, p = (natural[k, at, :] for k in range(4))
        outs[0][xi] = alpha * p
        outs[1][xi] = right[xi] - alpha * image
        outs[2][xi] = p - alpha * mw
        outs[3][xi] = image - alpha * nw


def pairs(count):
    return (
        [(i, i ^ 1) for i in range(count) if (i ^ 1) < count],
        [(i, ((i + 1) ^ 1) - 1) for i in range(1, count) if ((i + 1) ^ 1) - 1 < count],
    )


def turns(count):
    if count & (count - 1) == 0:
        return [[(i ^ t, i) for i in range(count)] for t in range(1, count)]
    return [[((i + t) % count, i) for i in range(count)] for t in range(1, count)]


def gather(block, axis, count):
    if count & (count - 1):
        return [block] + [lax.ppermute(block, axis, turn) for turn in turns(count)]
    found = {0: block}
    step = count // 2
    while step:
        turn = [(i, i ^ step) for i in range(count)]
        for t in list(found):
            found[t ^ step] = lax.ppermute(found[t], axis, turn)
        step //= 2
    return [found[t] for t in range(count)]


def shards(s, right_side, coefficient):
    L = s.bz
    ix, iy, iz = position()
    vmem = pl.BlockSpec(memory_space=pltpu.VMEM)
    struct = lambda *shape: jax.ShapeDtypeStruct(shape, f32)
    params = pltpu.CompilerParams(vmem_limit_bytes=16 * 4 * 2 * s.rows * s.slots * L)

    low = jnp.concatenate([right_side[:, :, : L // 2], coefficient[:, :, : L // 2]], axis=2)
    high = jnp.concatenate([right_side[:, :, L // 2:], coefficient[:, :, L // 2:]], axis=2)
    even_z = iz % 2 == 0
    send = (jnp.where(even_z, high, low), jnp.where(even_z, low, high))
    both = jnp.stack([right_side, coefficient])
    zpairs = pairs(s.nz)
    zside = [jnp.stack([lax.ppermute(v, "gz", p) for v, p in zip(send, zpairs)])]
    x_gc = []
    for turn in turns(s.nx):
        x_gc.append(lax.ppermute(both, "gx", turn))
        zside.append(lax.ppermute(zside[0], "gx", turn))

    def edge(rows):
        parts = []
        for t in range(s.nx):
            g, c = (right_side, coefficient) if t == 0 else (x_gc[t - 1][0], x_gc[t - 1][1])
            a, b = zside[t][0], zside[t][1]
            parts.append(jnp.concatenate([g[:, rows], c[:, rows]], axis=1))
            parts.append(jnp.concatenate([a[:, rows], b[:, rows]], axis=1))
        return jnp.stack(parts).reshape(s.nx, 2, s.bx, 2 * HALO, L)

    first_rows, last_rows = edge(slice(0, HALO)), edge(slice(s.by - HALO, s.by))
    even_y = iy % 2 == 0
    ypairs = pairs(s.ny)
    y_a = lax.ppermute(jnp.where(even_y, last_rows, first_rows), "gy", ypairs[0])
    y_b = lax.ppermute(jnp.where(even_y, first_rows, last_rows), "gy", ypairs[1])

    fine = struct(2, s.rows, s.slots, L)
    fine_scratch = pltpu.VMEM((2, s.rows, s.slots, L), f32)
    temps = pltpu.VMEM((2, 2, s.rows, s.slots, L), f32)
    temp1 = pltpu.VMEM(((s.bx // 2) * s.y1 * s.slots, L), f32)
    g, d, q, share = pl.pallas_call(
        lambda *refs: first_kernel(s, *refs),
        out_shape=(fine, fine, fine, struct(2, s.share, L)),
        in_specs=[vmem] * (2 + (s.nx - 1) + s.nx + 2),
        out_specs=(vmem,) * 4,
        scratch_shapes=[
            pltpu.VMEM((2, 4 * s.rows, 2 * L), f32),
            pltpu.VMEM((2, s.slots * s.rows, L), f32),
            pltpu.VMEM((2, s.slots * s.rows, L), f32),
            temps,
            temp1,
        ],
        compiler_params=params,
        name="widen",
    )(right_side, coefficient, *x_gc, *zside, y_a, y_b)

    spot = pltpu.VMEM((s.slots1 * s.rows1, L), f32)
    shares = gather(share, "gy", s.ny)
    p, image, d1, d2, share = pl.pallas_call(
        lambda *refs: second_kernel(s, *refs),
        out_shape=(
            fine,
            fine,
            struct(s.rows1, s.slots1, L),
            struct(s.rows1 // 4, s.slots1, L),
            struct(1, s.share + 2 * s.slots, L),
        ),
        in_specs=[vmem] * (s.ny + 3),
        out_specs=(vmem,) * 5,
        scratch_shapes=[spot, temps, temp1],
        compiler_params=params,
        name="cycle",
    )(*shares, g, d, q)

    shares = gather(share, "gy", s.ny)
    sums = sum(v[0, s.share:] for v in shares)
    sums = [sums] + [lax.ppermute(sums, "gz", turn) for turn in turns(s.nz)]
    natural = pl.pallas_call(
        lambda *refs: third_kernel(s, *refs),
        out_shape=struct(4, s.bx * s.by, L),
        in_specs=[vmem] * (s.ny + 6),
        out_specs=vmem,
        scratch_shapes=[
            spot,
            temps,
            pltpu.VMEM((2, s.rows * s.slots, L), f32),
            fine_scratch,
        ],
        compiler_params=params,
        name="again",
    )(*shares, p, image, d, q, d1, d2)
    return pl.pallas_call(
        lambda *refs: last_kernel(s, *refs),
        out_shape=(struct(s.bx, s.by, L),) * 4,
        in_specs=[vmem] * (s.nz + 2),
        out_specs=(vmem,) * 4,
        compiler_params=params,
        name="update",
    )(*sums, right_side, natural)


def solution(mesh):
    spec = P("gx", "gy", "gz")
    count = [mesh.shape[a] for a in ("gx", "gy", "gz")]

    def body(right_side, coefficient):
        s = Shape(*count, right_side.shape)
        assert s.bx % 4 == 0 and s.by % 16 == 0 and s.bz % 128 == 0
        return shards(s, right_side, coefficient)

    return jax.shard_map(
        body, mesh=mesh, in_specs=(spec, spec), out_specs=(spec,) * 4, check_vma=False
    )
```

```python
import jax
import jax.numpy as jnp
from jax import lax
from jax.experimental import pallas as pl
from jax.experimental.pallas import tpu as pltpu
from jax.sharding import PartitionSpec as P


SWEEPS = 4
relaxation = 0.6
f32 = jnp.float32

HALO = 4
COLUMNS = 40


def roll(value, shift, axis):
    return pltpu.roll(value, shift % value.shape[axis], axis)


def position():
    return tuple(lax.axis_index(a) for a in ("gx", "gy", "gz"))


def iota(shape, axis):
    return lax.broadcasted_iota(jnp.int32, shape, axis)


class Shape:
    def __init__(self, nx, ny, nz, block):
        self.nx, self.ny, self.nz = nx, ny, nz
        self.bx, self.by, self.bz = block
        self.half = self.by // 2
        self.slots = nx * 4
        self.rows = self.bx * self.half
        self.x1 = nx * self.bx // 2
        self.y1 = self.half // 2
        self.slots1 = 2 * ny
        self.rows1 = self.x1 * self.y1
        self.share = 2 * self.rows1
        self.group = self.bz // COLUMNS
        self.packs = -(-self.bx // self.group)


def fine_tools(s):
    shape = (s.slots, s.bz)
    sub = iota(shape, 0)
    first_block = sub < 4
    last_block = sub >= s.slots - 4
    first_chunk = sub % 4 == 0
    last_chunk = sub % 4 == 3

    def below_x(v):
        return jnp.where(first_block, 0.0, roll(v, 4, 0))

    def above_x(v):
        return jnp.where(last_block, 0.0, roll(v, -4, 0))

    def below_y(v):
        return jnp.where(first_chunk, 0.0, roll(v, 1, 0))

    def above_y(v):
        return jnp.where(last_chunk, 0.0, roll(v, -1, 0))

    return below_x, above_x, below_y, above_y


def triple(v, low, high):
    n = len(v)
    out = []
    for i in range(0, n, 2):
        pair = v[i] + v[i + 1]
        out.append(pair + (low if i == 0 else v[i - 1]))
        out.append(pair + (high if i + 2 == n else v[i + 2]))
    return out


def plain_triple(v):
    n = len(v)
    out = []
    for i in range(n):
        total = v[i]
        if i > 0:
            total = total + v[i - 1]
        if i + 1 < n:
            total = total + v[i + 1]
        out.append(total)
    return out


def fine_block_sum(s, source, temp, consume):
    below_x, above_x, below_y, above_y = fine_tools(s)
    for par in range(2):
        for yi in range(s.half):
            v = [source[par, xi * s.half + yi] for xi in range(s.bx)]
            for xi, t in enumerate(triple(v, below_x(v[-1]), above_x(v[0]))):
                temp[par, xi * s.half + yi] = t
    for i in range(s.bx // 2):
        sums = []
        for k in range(2):
            xi = 2 * i + k
            both = []
            for par in range(2):
                v = [temp[par, xi * s.half + yi] for yi in range(s.half)]
                both.append(triple(v, below_y(v[-1]), above_y(v[0])))
            even, odd = both
            out_even, out_odd = [], []
            for e, o in zip(even, odd):
                pair = e + o
                out_even.append(pair + roll(o, 1, 1))
                out_odd.append(pair + roll(e, -1, 1))
            sums.append((out_even, out_odd))
        consume(i, sums)


def fine_restrict(s, values, i, store):
    for j in range(s.y1):
        total = None
        for k in range(2):
            for par in range(2):
                for yi in (2 * j, 2 * j + 1):
                    v = values[k][par][yi]
                    total = v if total is None else total + v
        store(i * s.y1 + j, 0.5 * total)


def split3(v):
    high = v.astype(jnp.bfloat16)
    rest = v - high.astype(f32)
    middle = rest.astype(jnp.bfloat16)
    low = (rest - middle.astype(f32)).astype(jnp.bfloat16)
    return high, middle, low


def exact_dot(v, selection):
    dot = lambda a: jnp.dot(a, selection, preferred_element_type=f32)
    high, middle, low = split3(v)
    return dot(high) + (dot(middle) + dot(low))


def share_out(s, temp, out):
    count = (s.bx // 2) * s.y1
    for h in range(2):
        for b in range(s.nx):
            out[pl.ds(h * s.rows1 + b * count, count), :] = temp[
                pl.ds(b * 4 + 1 + h, count, stride=s.slots), :
            ]


def pack_kernel(s, both, send_a, send_b):
    iz = position()[2]
    even = iz % 2 == 0
    shape = (s.by, s.bz)
    lane = iota(shape, 1)
    for arr in range(2):
        for pack in range(s.packs):
            first = jnp.zeros(shape, f32)
            last = jnp.zeros(shape, f32)
            for m in range(min(s.group, s.bx - pack * s.group)):
                xi = pack * s.group + m
                v = both[arr, xi]
                here = (lane >= m * COLUMNS) & (lane < (m + 1) * COLUMNS)
                first = jnp.where(here, roll(v, m * COLUMNS, 1) if m else v, first)
                last = jnp.where(here, roll(v, (m + 1) * COLUMNS, 1), last)
            send_a[arr, pack] = jnp.where(even, last, first)
            send_b[arr, pack] = jnp.where(even, first, last)


def column_tools(s, rows):
    even_z = position()[2] % 2 == 0
    lane = iota((rows, s.bz), 1)
    front = lane < COLUMNS
    back = lane >= s.bz - COLUMNS

    def halo(xi, a, b):
        at = (xi % s.group) * COLUMNS
        following = jnp.where(even_z, a, b)
        previous = jnp.where(even_z, b, a)
        following = roll(following, -at, 1) if at else following
        previous = roll(previous, s.bz - COLUMNS - at, 1)
        return jnp.where(front, following, jnp.where(back, previous, 0.0))

    shape = (2 * s.bz, 2 * s.bz)
    source, target = iota(shape, 0), iota(shape, 1)
    wanted = jnp.where(target < s.bz, 2 * target, 2 * (target - s.bz) + 1)
    selection = jnp.where(source == wanted, 1.0, 0.0).astype(jnp.bfloat16)
    return halo, selection


def block_of(s, ix, t):
    return (ix ^ t) if s.nx & (s.nx - 1) == 0 else (ix + t) % s.nx


def own_kernel(s, *refs):
    n = s.nx
    blocks, sides = refs[:n], refs[n:2 * n]
    split, share, natural, temp = refs[2 * n:]
    ix = position()[0]
    L = s.bz
    halo, selection = column_tools(s, s.half)
    count = (s.bx // 2) * s.y1
    for t in range(n):
        b = block_of(s, ix, t)
        for arr in range(2):
            for h in range(2):
                span = pl.ds(h * s.half, s.half)
                for xi in range(s.bx):
                    at = pl.ds(h * s.rows + xi * s.half, s.half)
                    a = sides[t][0, arr, xi // s.group, span, :]
                    z = sides[t][1, arr, xi // s.group, span, :]
                    natural[at, pl.ds(0, L)] = blocks[t][arr, xi, span, :]
                    natural[at, pl.ds(L, L)] = halo(xi, a, z)
            parted = exact_dot(natural[...], selection)
            start = pl.multiple_of((b * 4 + 1) * s.rows, s.rows)
            for par in range(2):
                split[arr, par, pl.ds(start, 2 * s.rows), :] = parted[:, par * L:(par + 1) * L]
            if arr == 0:
                continue
            for h in range(2):
                for i in range(s.bx // 2):
                    at = h * s.rows + 2 * i * s.half
                    low, high = parted[at:at + s.half], parted[at + s.half:at + 2 * s.half]
                    total = (low[:, :L] + low[:, L:]) + (high[:, :L] + high[:, L:])
                    temp[pl.ds(i * s.half, s.half), :] = 0.5 * (total + roll(total, -1, 0))
                to = pl.multiple_of(h * s.rows1 + b * count, count)
                share[pl.ds(to, count), :] = temp[pl.ds(0, count, stride=2), :]


def first_kernel(s, *refs):
    blocks_a, blocks_b, sides_a, sides_b, _ = refs[:5]
    split, g_out, d_out, q_out, share, natural, temp, temp1 = refs[5:]
    ix, iy, iz = position()
    even_y = iy % 2 == 0
    L = s.bz
    halo, selection = column_tools(s, 2 * HALO)
    row = iota((s.half, L), 0)
    for ch in (0, 3):
        use_a = even_y if ch == 3 else jnp.logical_not(even_y)
        for t in range(s.nx):
            for xi in range(s.bx):
                at = pl.ds((t * s.bx + xi) * 2 * HALO, 2 * HALO)
                pack = xi // s.group
                a = jnp.where(use_a, sides_a[t, 0, pack], sides_b[t, 0, pack])
                z = jnp.where(use_a, sides_a[t, 1, pack], sides_b[t, 1, pack])
                natural[at, pl.ds(0, L)] = jnp.where(use_a, blocks_a[t, xi], blocks_b[t, xi])
                natural[at, pl.ds(L, L)] = halo(xi, a, z)
        parted = exact_dot(natural[...], selection)
        for t in range(s.nx):
            b = block_of(s, ix, t)
            for xi in range(s.bx):
                at = (t * s.bx + xi) * 2 * HALO
                to = pl.multiple_of((b * 4 + ch) * s.rows + xi * s.half, s.half)
                for par in range(2):
                    v = parted[at:at + 2 * HALO, par * L:(par + 1) * L]
                    turned = roll(v, HALO, 0)
                    g, c = (v, turned) if ch == 3 else (turned, v)
                    split[0, par, pl.ds(to, s.half), :] = g
                    split[1, par, pl.ds(to, s.half), :] = c

    shape = (s.slots, L)
    subs = iota(shape, 0) % 4
    inside = inside_columns(s, iz, shape) & inside_chunks(s, iy, subs)
    for par in range(2):
        for r in range(s.rows):
            yi = r % s.half
            q = 26.0 + split[1, par, pl.ds(r, s.slots, stride=s.rows), :]
            valid = inside
            if yi >= HALO:
                valid = valid & (subs != 3)
            if yi < s.half - HALO:
                valid = valid & (subs != 0)
            g = split[0, par, pl.ds(r, s.slots, stride=s.rows), :]
            g_out[par, r] = jnp.where(valid, g, 0.0)
            q_out[par, r] = q
            d_out[par, r] = jnp.where(valid, relaxation / q, 0.0)
    first_half(s, g_out, d_out, temp, temp1, share)


def first_half(s, g_ref, d_ref, temps, temp1, share):
    e_ref, x_ref = temps.at[0], temps.at[1]
    for par in range(2):
        for r in range(s.rows):
            e_ref[par, r] = d_ref[par, r] * g_ref[par, r]

    def consume(i, sums):
        values = []
        for k in range(2):
            both = []
            for par in range(2):
                line = []
                for yi in range(s.half):
                    r = (2 * i + k) * s.half + yi
                    line.append(
                        (1.0 - relaxation) * g_ref[par, r] - e_ref[par, r] + sums[k][par][yi]
                    )
                both.append(line)
            values.append(both)

        def keep(at, tile1):
            temp1[pl.ds(at * s.slots, s.slots), :] = tile1

        fine_restrict(s, values, i, keep)

    fine_block_sum(s, e_ref, x_ref, consume)
    share_out(s, temp1, share)


def gather_shares(s, iy, shares, spot):
    for t, ref in enumerate(shares):
        at = (iy ^ t) if s.ny & (s.ny - 1) == 0 else (iy + t) % s.ny
        start = pl.multiple_of(at * s.share, s.share)
        spot[pl.ds(start, s.share), :] = ref[pl.ds(0, s.share), :]
    return [spot[pl.ds(r, s.slots1, stride=s.rows1), :] for r in range(s.rows1)]


def middle_sum(v, nx, ny, step):
    shape = v[0].shape
    sub = iota(shape, 0)
    first, last = sub == 0, sub == shape[0] - 1
    out = [None] * (nx * ny)
    for yi in range(ny):
        for xi, t in enumerate(plain_triple([v[x * ny + yi] for x in range(nx)])):
            out[xi * ny + yi] = t
    for xi in range(nx):
        line = out[xi * ny:(xi + 1) * ny]
        low = jnp.where(first, 0.0, roll(line[-1], 1, 0))
        high = jnp.where(last, 0.0, roll(line[0], -1, 0))
        out[xi * ny:(xi + 1) * ny] = triple(line, low, high)
    return [t + (roll(t, step, 1) + roll(t, -step, 1)) for t in out]


def middle_restrict(s, v):
    out = []
    for i in range(s.x1 // 2):
        for j in range(s.y1 // 2):
            t = (v[2 * i * s.y1 + 2 * j] + v[2 * i * s.y1 + 2 * j + 1]) + (
                v[(2 * i + 1) * s.y1 + 2 * j] + v[(2 * i + 1) * s.y1 + 2 * j + 1]
            )
            out.append(0.5 * (t + roll(t, -1, 1)))
    return out


def inside_columns(s, iz, shape):
    lanes = iota(shape, 1)
    below = jnp.where(iz < s.nz - 1, (s.bz + COLUMNS) // 2, s.bz // 2)
    above = jnp.where(iz > 0, s.bz - COLUMNS // 2, s.bz)
    return (lanes < below) | (lanes >= above)


def inside_chunks(s, iy, chunk):
    first = jnp.where(iy > 0, 0, 1)
    last = jnp.where(iy < s.ny - 1, 3, 2)
    return (chunk >= first) & (chunk <= last)


def middle_solve(s, g, d1, d2):
    keep = 1.0 - relaxation
    e0 = [d * t for d, t in zip(d1, g)]
    sums = middle_sum(e0, s.x1, s.y1, 1)
    g2 = middle_restrict(s, [keep * t - e + u for t, e, u in zip(g, e0, sums)])
    e = [d * t for d, t in zip(d2, g2)]
    for _ in range(SWEEPS - 1):
        sums = middle_sum(e, s.x1 // 2, s.y1 // 2, 2)
        e = [keep * a + d * ((t - a) + u) for a, d, t, u in zip(e, d2, g2, sums)]
    spread = [a + roll(a, 1, 1) for a in e]
    e1 = [
        e0[x * s.y1 + y] + spread[(x // 2) * (s.y1 // 2) + y // 2]
        for x in range(s.x1)
        for y in range(s.y1)
    ]
    sums = middle_sum(e1, s.x1, s.y1, 1)
    return [keep * a + d * ((t - a) + u) for a, d, t, u in zip(e1, d1, g, sums)]


def to_fine(s, iy, e2):
    shape = (s.slots, s.bz)
    sub = iota(shape, 0)
    block = sub // 4
    chunk = sub % 4
    known = inside_chunks(s, iy, chunk)
    out = []
    per = s.bx // 2
    for x in range(per):
        for y in range(s.y1):
            total = jnp.zeros(shape, f32)
            for b in range(s.nx):
                v = e2[(b * per + x) * s.y1 + y]
                shift = (4 * b + 1 - 2 * iy) % s.slots1
                if s.slots1 < s.slots:
                    v = jnp.concatenate([v] * (s.slots // s.slots1), axis=0)
                v = pltpu.roll(v, shift, 0)[: s.slots]
                total = jnp.where(block == b, v, total)
            out.append(jnp.where(known, total, 0.0))
    return out


def second_half(s, g_ref, d_ref, q_ref, coarse, e_ref, x_ref, p_ref, image_store):
    for par in range(2):
        for xi in range(s.bx):
            for yi in range(s.half):
                r = xi * s.half + yi
                e_ref[par, r] = (
                    d_ref[par, r] * g_ref[par, r] + coarse[(xi // 2) * s.y1 + yi // 2]
                )

    def smooth(i, sums):
        for k in range(2):
            for par in range(2):
                for yi in range(s.half):
                    r = (2 * i + k) * s.half + yi
                    e = e_ref[par, r]
                    p_ref[par, r] = (1.0 - relaxation) * e + d_ref[par, r] * (
                        (g_ref[par, r] - e) + sums[k][par][yi]
                    )

    fine_block_sum(s, e_ref, x_ref, smooth)

    def apply(i, sums):
        for k in range(2):
            for par in range(2):
                for yi in range(s.half):
                    r = (2 * i + k) * s.half + yi
                    p = p_ref[par, r]
                    image_store(par, r, (q_ref[par, r] * p + p) - sums[k][par][yi])

    fine_block_sum(s, p_ref, x_ref, apply)


def second_kernel(s, *refs):
    shares, shares_c = refs[: s.ny], refs[s.ny:2 * s.ny]
    refs = refs[2 * s.ny:]
    g_ref, d_ref, q_ref, p_out, image_out, d1_out, d2_out, share = refs[:8]
    spot, temps, temp1 = refs[8:]
    _, iy, iz = position()
    g1 = gather_shares(s, iy, shares, spot)
    c1 = gather_shares(s, iy, shares_c, spot)
    shape = (s.slots1, s.bz)
    inside = inside_columns(s, iz, shape)
    inside2 = inside & (iota(shape, 1) % 2 == 0)
    d1 = [jnp.where(inside, relaxation / (26.0 + c), 0.0) for c in c1]
    d2 = [jnp.where(inside2, relaxation / (26.0 + c), 0.0) for c in middle_restrict(s, c1)]
    for r, d in enumerate(d1):
        d1_out[r] = d
    for r, d in enumerate(d2):
        d2_out[r] = d
    coarse = to_fine(s, iy, middle_solve(s, g1, d1, d2))
    e_ref, x_ref = temps.at[0], temps.at[1]

    def keep(par, r, value):
        image_out[par, r] = value

    second_half(s, g_ref, d_ref, q_ref, coarse, e_ref, x_ref, p_out, keep)
    shape = (s.slots, s.bz)
    chunk = iota(shape, 0) % 4
    own = (iota(shape, 1) < s.bz // 2) & (chunk > 0) & (chunk < 3)
    gammas = [jnp.zeros(shape, f32) for _ in range(4)]
    deltas = [jnp.zeros(shape, f32) for _ in range(4)]
    for par in range(2):
        for r in range(s.rows):
            p = p_out[par, r]
            gammas[r % 4] += g_ref[par, r] * p
            deltas[r % 4] += image_out[par, r] * p
    gamma = jnp.where(own, (gammas[0] + gammas[1]) + (gammas[2] + gammas[3]), 0.0)
    delta = jnp.where(own, (deltas[0] + deltas[1]) + (deltas[2] + deltas[3]), 0.0)
    share[pl.ds(s.share, s.slots), :] = gamma
    share[pl.ds(s.share + s.slots, s.slots), :] = delta
    first_half(s, image_out, d_ref, temps, temp1, share)


def third_kernel(s, *refs):
    shares = refs[: s.ny]
    p_ref, g_ref, d_ref, q_ref, d1_ref, d2_ref, out = refs[s.ny:s.ny + 7]
    spot, temps, flat, mw_ref = refs[s.ny + 7:]
    ix, iy, _ = position()
    g1 = gather_shares(s, iy, shares, spot)
    d1 = [d1_ref[r] for r in range(s.rows1)]
    d2 = [d2_ref[r] for r in range(s.rows1 // 4)]
    coarse = to_fine(s, iy, middle_solve(s, g1, d1, d2))
    e_ref, x_ref = temps.at[0], temps.at[1]

    def keep(par, r, value):
        flat[par, pl.ds(r * s.slots, s.slots), :] = value

    second_half(s, g_ref, d_ref, q_ref, coarse, e_ref, x_ref, mw_ref, keep)
    L = s.bz
    source = iota((L, L), 0)
    target = iota((L, L), 1)
    wanted = jnp.where(target % 2 == 0, target // 2, L // 2 + target // 2)
    selection = jnp.where(source == wanted, 1.0, 0.0).astype(jnp.bfloat16)
    left = iota((s.half, L), 1) < L // 2
    for k, ref in enumerate((None, mw_ref, g_ref, p_ref)):
        if ref is not None:
            for par in range(2):
                for r in range(s.rows):
                    flat[par, pl.ds(r * s.slots, s.slots), :] = ref[par, r]
        tiles = []
        for xi in range(s.bx):
            for h in range(2):
                at = xi * s.half * s.slots + ix * 4 + 1 + h
                even = flat[0, pl.ds(at, s.half, stride=s.slots), :]
                odd = flat[1, pl.ds(at, s.half, stride=s.slots), :]
                tiles.append(jnp.where(left, even, roll(odd, L // 2, 1)))
        out[k] = exact_dot(jnp.concatenate(tiles, axis=0), selection)


def last_kernel(s, *refs):
    right, natural = refs[s.nz:s.nz + 2]
    outs = refs[s.nz + 2:]
    total = refs[0][...]
    for v in refs[1:s.nz]:
        total = total + v[...]
    gamma = jnp.sum(total[: s.slots], keepdims=True)
    delta = jnp.sum(total[s.slots:], keepdims=True)
    alpha = gamma / delta
    for xi in range(s.bx):
        at = pl.ds(xi * s.by, s.by)
        nw, mw, image, p = (natural[k, at, :] for k in range(4))
        outs[0][xi] = alpha * p
        outs[1][xi] = right[xi] - alpha * image
        outs[2][xi] = p - alpha * mw
        outs[3][xi] = image - alpha * nw


def pairs(count, closed=False):
    even = [(i, i + 1) for i in range(0, count - 1, 2)]
    odd = [(i, (i + 1) % count) for i in range(1, count if closed and count > 2 else count - 1, 2)]
    return [[p for i, j in swaps for p in ((i, j), (j, i))] for swaps in (even, odd)]


def filled(others, count, swaps):
    idle = set(range(count)) - {i for i, _ in swaps}
    if others % 2:
        idle = set()
    return [
        (other * count + i, other * count + j) for other in range(others) for i, j in swaps
    ] + [(other * count + i, (other ^ 1) * count + i) for other in range(others) for i in sorted(idle)]


def turns(count):
    if count & (count - 1) == 0:
        return [[(i ^ t, i) for i in range(count)] for t in range(1, count)]
    return [[((i + t) % count, i) for i in range(count)] for t in range(1, count)]


def gather(block, axis, count):
    if count & (count - 1):
        return [block] + [lax.ppermute(block, axis, turn) for turn in turns(count)]
    found = {0: block}
    step = count // 2
    while step:
        turn = [(i, i ^ step) for i in range(count)]
        for t in list(found):
            found[t ^ step] = lax.ppermute(found[t], axis, turn)
        step //= 2
    return [found[t] for t in range(count)]


def shards(s, right_side, coefficient):
    L = s.bz
    vmem = pl.BlockSpec(memory_space=pltpu.VMEM)
    struct = lambda *shape: jax.ShapeDtypeStruct(shape, f32)
    params = pltpu.CompilerParams(vmem_limit_bytes=16 * 4 * 2 * s.rows * s.slots * L)

    pack = struct(2, s.packs, s.by, L)
    both = jnp.stack([right_side, coefficient])
    send_a, send_b = pl.pallas_call(
        lambda *refs: pack_kernel(s, *refs),
        out_shape=(pack, pack),
        in_specs=[vmem],
        out_specs=(vmem,) * 2,
        compiler_params=params,
        name="pack",
    )(both)
    blocks = [both] + [lax.ppermute(both, "gx", turn) for turn in turns(s.nx)]
    received = [
        lax.ppermute(v, ("gy", "gz"), filled(s.ny, s.nz, p))
        for v, p in zip((send_a, send_b), pairs(s.nz))
    ]
    side = jnp.stack(received)
    sides = [side] + [lax.ppermute(side, "gx", turn) for turn in turns(s.nx)]

    even_y = position()[1] % 2 == 0
    first_rows, last_rows = slice(0, HALO), slice(s.by - HALO, s.by)

    def swap_rows(values):
        edges = [
            jnp.concatenate([values[0][..., rows, :], values[1][..., rows, :]], axis=-2)
            for rows in (first_rows, last_rows)
        ]
        a, b = pairs(s.ny, s.ny % 2 == 0)
        return (
            lax.ppermute(jnp.where(even_y, edges[1], edges[0]), "gy", a),
            lax.ppermute(jnp.where(even_y, edges[0], edges[1]), "gy", b),
        )

    stacked = jnp.stack(blocks, axis=1)
    blocks_a, blocks_b = swap_rows((stacked[0], stacked[1]))
    stacked = jnp.stack(sides)
    sides_a, sides_b = swap_rows((stacked[:, :, 0], stacked[:, :, 1]))

    fine = struct(2, s.rows, s.slots, L)
    fine_scratch = pltpu.VMEM((2, s.rows, s.slots, L), f32)
    temps = pltpu.VMEM((2, 2, s.rows, s.slots, L), f32)
    temp1 = pltpu.VMEM(((s.bx // 2) * s.y1 * s.slots, L), f32)
    split_shape = struct(2, 2, s.slots * s.rows, L)
    share_shape = struct(s.share, L)
    split, share = pl.pallas_call(
        lambda *refs: own_kernel(s, *refs),
        out_shape=(split_shape, share_shape),
        in_specs=[vmem] * (2 * s.nx),
        out_specs=(vmem,) * 2,
        scratch_shapes=[
            pltpu.VMEM((2 * s.rows, 2 * L), f32),
            pltpu.VMEM((s.bx // 2 * s.half, L), f32),
        ],
        compiler_params=params,
        name="own",
    )(*blocks, *sides)
    shares_c = gather(share, "gy", s.ny)
    _, g, d, q, share = pl.pallas_call(
        lambda *refs: first_kernel(s, *refs),
        out_shape=(split_shape, fine, fine, fine, share_shape),
        in_specs=[vmem] * 5,
        out_specs=(vmem,) * 5,
        input_output_aliases={4: 0},
        scratch_shapes=[
            pltpu.VMEM((s.nx * s.bx * 2 * HALO, 2 * L), f32),
            temps,
            temp1,
        ],
        compiler_params=params,
        name="widen",
    )(blocks_a, blocks_b, sides_a, sides_b, split)

    spot = pltpu.VMEM((s.slots1 * s.rows1, L), f32)
    shares = gather(share, "gy", s.ny)
    p, image, d1, d2, share = pl.pallas_call(
        lambda *refs: second_kernel(s, *refs),
        out_shape=(
            fine,
            fine,
            struct(s.rows1, s.slots1, L),
            struct(s.rows1 // 4, s.slots1, L),
            struct(s.share + 2 * s.slots, L),
        ),
        in_specs=[vmem] * (2 * s.ny + 3),
        out_specs=(vmem,) * 5,
        scratch_shapes=[spot, temps, temp1],
        compiler_params=params,
        name="cycle",
    )(*shares, *shares_c, g, d, q)

    shares = gather(share, "gy", s.ny)
    part = sum(v[s.share:] for v in shares)
    sums = [part] + [lax.ppermute(part, "gz", turn) for turn in turns(s.nz)]
    natural = pl.pallas_call(
        lambda *refs: third_kernel(s, *refs),
        out_shape=struct(4, s.bx * s.by, L),
        in_specs=[vmem] * (s.ny + 6),
        out_specs=vmem,
        scratch_shapes=[
            spot,
            temps,
            pltpu.VMEM((2, s.rows * s.slots, L), f32),
            fine_scratch,
        ],
        compiler_params=params,
        name="again",
    )(*shares, p, image, d, q, d1, d2)
    return pl.pallas_call(
        lambda *refs: last_kernel(s, *refs),
        out_shape=(struct(s.bx, s.by, L),) * 4,
        in_specs=[vmem] * (s.nz + 2),
        out_specs=(vmem,) * 4,
        compiler_params=params,
        name="update",
    )(*sums, right_side, natural)


def solution(mesh):
    spec = P("gx", "gy", "gz")
    count = [mesh.shape[a] for a in ("gx", "gy", "gz")]

    def body(right_side, coefficient):
        s = Shape(*count, right_side.shape)
        assert s.bx % 4 == 0 and s.by % 16 == 0 and s.bz % 128 == 0
        return shards(s, right_side, coefficient)

    return jax.shard_map(
        body, mesh=mesh, in_specs=(spec, spec), out_specs=(spec,) * 4, check_vma=False
    )
```
